256 devices in a mesh: ctx: 32 (over x, y, core), head: 8 (over z).
Axes of the slice: x: 4, y: 4, z: 8, core: 2. Of those that a mesh axis runs over, the one named last changes fastest.
Arguments:
- queries: bfloat16 [8192, 8192], P(('ctx', 'head')), may hold values from -6 to 6
- key_heads: bfloat16 [8192, 1024], P(('ctx', 'head')), may hold values from -6 to 6
- value_head_array: bfloat16 [8192, 1024], P(('ctx', 'head')), may hold values from -6 to 6
- out_grad: bfloat16 [8192, 8192], P(('ctx', 'head')), may hold values from -6 to 6
- doc_ids: int32 [8192], P('ctx'), may hold values from 0 to 127, never falling along the last dimension, each value on 1 to 1792 neighbouring positions
Outputs:
- attended: bfloat16 [8192, 8192], P(('ctx', 'head'))
- query_grad: bfloat16 [8192, 8192], P(('ctx', 'head'))
- key_grad: bfloat16 [8192, 1024], P(('ctx', 'head'))
- value_grad: bfloat16 [8192, 1024], P(('ctx', 'head'))
The draws below stay inside these ranges and needn't reach their ends.
Inputs may be any that keep to these rules, and one draw needn't show every extreme that they name: `doc_ids`: document numbers never fall along the batch; each document holds 1 to 1792 consecutive tokens and one holds exactly 1792.
All inputs are finite; a program needn't handle non-finite values.
Results may differ from the reference program's by a relative error of at most 0.022.
Values may be sent and summed in bfloat16 or wider, within the bound.
No kernel may reach another device: no remote copies, remote signals or barrier semaphores. Data moves between devices by JAX's collectives and lax.ppermute only.
A program may use at most 128 MiB of HBM per device.

```python
import math
import jax
import jax.numpy as jnp
import numpy as np
from jax import lax

QUERY_HEADS = 64
KEY_VALUE_HEADS = 8
HEAD_SIZE = 128
WINDOW = 1536
PACKED_TOKENS = 8192
DOCS = 128
DOC_MOST = 1792


def paired_fields(key):
    folded = jax.random.fold_in(key, 11)
    random_subkeys = jax.random.split(folded, 2)
    query_all = jnp.clip(jax.random.normal(random_subkeys[0], (PACKED_TOKENS, QUERY_HEADS * HEAD_SIZE), jnp.float32), -6.0, 6.0)
    every_key = jnp.clip(jax.random.normal(random_subkeys[1], (PACKED_TOKENS, KEY_VALUE_HEADS * HEAD_SIZE), jnp.float32), -6.0, 6.0)
    return (query_all, every_key)


def draw_queries(key, part):
    return paired_fields(key)[0].astype(jnp.bfloat16)


def draw_key_heads(key, part):
    return paired_fields(key)[1].astype(jnp.bfloat16)


def block_scale(stream_key, shape, shards, low, high):
    def one(position, blocks):
        steps = jax.random.uniform(jax.random.fold_in(jax.random.fold_in(stream_key, 6), position), (blocks,), jnp.float32, low / len(shards), high / len(shards))
        return jnp.repeat(jnp.exp(steps), shape[position] // blocks).reshape((-1,) + (1,) * (len(shape) - position - 1))

    factor_of = one(*shards[0])
    for cut in shards[1:]:
        factor_of = factor_of * one(*cut)
    return factor_of


def length_profile(number_of, total, limit, lean):
    weights = [(1 << 20) // math.isqrt(grade ** lean) + 1 for grade in range(2, number_of + 1)]
    spare, holding = total - limit - (number_of - 1), [1] * (number_of - 1)
    while spare > 0:
        candidates = [i for i in range(number_of - 1) if holding[i] < limit]
        pool, left = sum([weights[i] for i in candidates]), spare
        for i in candidates:
            more = min(limit - holding[i], max(1, left * weights[i] // pool), spare)
            holding[i] = holding[i] + more
            spare = spare - more
    return np.array([limit] + holding)


def uneven_parts(key, amount, total, bound, slope):
    if amount == 2:
        one = jax.random.randint(key, (), max(1, total - bound), min(bound, total - 1) + 1)
        return jnp.stack([one, total - one])
    sizes = jnp.asarray(length_profile(amount, total, bound, slope), jnp.int32)
    pairs = (amount - 1) // 2
    giver, sink = sizes[1:1 + 2 * pairs:2], sizes[2:2 + 2 * pairs:2]
    room = jnp.minimum(giver - 1, bound - sink)
    shifted = jax.random.randint(jax.random.fold_in(key, 1), (pairs,), 0, 1 << 20) % (room + 1)
    sizes = sizes.at[1:1 + 2 * pairs:2].set(giver - shifted).at[2:2 + 2 * pairs:2].set(sink + shifted)
    return sizes[jax.random.permutation(jax.random.fold_in(key, 2), amount)]


def scatter_about(own_key, dims, deviation, limit, shards=(), kind=jnp.bfloat16):
    result = deviation * jax.random.normal(own_key, dims, jnp.float32)
    if shards:
        result = result * block_scale(own_key, dims, shards, -0.22, 0.18)
    return jnp.clip(result, -limit, limit).astype(kind)


def setup_inputs(seed: int = 0) -> dict:
    arg_keys = jax.random.split(jax.random.key(seed), 6)
    return {
        "queries": draw_queries(jax.random.fold_in(arg_keys[5], 71), 0),
        "key_heads": draw_key_heads(jax.random.fold_in(arg_keys[5], 71), 0),
        "value_head_array": scatter_about(arg_keys[2], (PACKED_TOKENS, KEY_VALUE_HEADS * HEAD_SIZE), 1.0, 6.0, ((0, 256),)),
        "out_grad": scatter_about(arg_keys[3], (PACKED_TOKENS, QUERY_HEADS * HEAD_SIZE), 1.0, 6.0, ((0, 256),)),
        "doc_ids": jnp.searchsorted(jnp.cumsum(uneven_parts(arg_keys[4], DOCS, PACKED_TOKENS, DOC_MOST, 2)), jnp.arange(PACKED_TOKENS), side="right").astype(jnp.int32),
    }


def reference(queries, key_heads, value_head_array, out_grad, doc_ids):
    total_rows = queries.shape[0]
    kv_width = key_heads.shape[1]
    kv_heads = kv_width // HEAD_SIZE
    group_size = queries.shape[1] // kv_width
    block_rows = math.gcd(total_rows, 128)
    key_span = block_rows + WINDOW
    score_scale = HEAD_SIZE ** -0.5
    key_pad = jnp.concatenate([jnp.zeros((WINDOW, kv_width), key_heads.dtype), key_heads], axis=0)
    value_pad = jnp.concatenate([jnp.zeros((WINDOW, kv_width), value_head_array.dtype), value_head_array], axis=0)
    doc_pad = jnp.concatenate([jnp.full((WINDOW,), -1, jnp.int32), doc_ids.astype(jnp.int32)])

    def step(carry, block_index):
        key_acc, value_acc = carry
        first_row = (block_index * block_rows).astype(jnp.int32)
        query_four = lax.dynamic_slice_in_dim(queries, first_row, block_rows, 0).astype(jnp.float32).reshape(block_rows, kv_heads, group_size, HEAD_SIZE)
        grad_four = lax.dynamic_slice_in_dim(out_grad, first_row, block_rows, 0).astype(jnp.float32).reshape(block_rows, kv_heads, group_size, HEAD_SIZE)
        key_three = lax.dynamic_slice_in_dim(key_pad, first_row, key_span, 0).astype(jnp.float32).reshape(key_span, kv_heads, HEAD_SIZE)
        value_three = lax.dynamic_slice_in_dim(value_pad, first_row, key_span, 0).astype(jnp.float32).reshape(key_span, kv_heads, HEAD_SIZE)
        query_pos = first_row + jnp.arange(block_rows, dtype=jnp.int32)
        key_pos = first_row - WINDOW + jnp.arange(key_span, dtype=jnp.int32)
        query_doc = lax.dynamic_slice_in_dim(doc_ids.astype(jnp.int32), first_row, block_rows, 0)
        key_doc = lax.dynamic_slice_in_dim(doc_pad, first_row, key_span, 0)
        distance = query_pos[:, None] - key_pos[None, :]
        visible = (query_doc[:, None] == key_doc[None, :]) & (key_pos[None, :] >= 0) & (distance >= 0) & (distance < WINDOW)
        scores = jnp.einsum("qgpd,kgd->gpqk", query_four, key_three) * score_scale
        masked = jnp.where(visible, scores, -jnp.inf)
        row_max = jnp.max(masked, axis=-1, keepdims=True)
        log_total = row_max + jnp.log(jnp.sum(jnp.where(visible, jnp.exp(masked - row_max), 0.0), axis=-1, keepdims=True))
        prob_block = jnp.where(visible, jnp.exp(scores - log_total), 0.0)
        weights = prob_block.astype(jnp.bfloat16).astype(jnp.float32)
        out_rounded = jnp.einsum("gpqk,kgd->qgpd", weights, value_three).astype(jnp.bfloat16)
        row_delta = jnp.einsum("qgpd,qgpd->gpq", grad_four, out_rounded.astype(jnp.float32))[..., None]
        prob_grad = jnp.einsum("qgpd,kgd->gpqk", grad_four, value_three)
        score_grad = (prob_block * (prob_grad - row_delta)).astype(jnp.bfloat16).astype(jnp.float32)
        query_rows = (score_scale * jnp.einsum("gpqk,kgd->qgpd", score_grad, key_three)).astype(jnp.bfloat16)
        key_term = score_scale * jnp.einsum("gpqk,qgpd->kgd", score_grad, query_four)
        value_term = jnp.einsum("gpqk,qgpd->kgd", weights, grad_four)
        key_old = lax.dynamic_slice_in_dim(key_acc, first_row, key_span, 0)
        value_old = lax.dynamic_slice_in_dim(value_acc, first_row, key_span, 0)
        key_acc = lax.dynamic_update_slice_in_dim(key_acc, key_old + key_term.reshape(key_span, kv_width), first_row, 0)
        value_acc = lax.dynamic_update_slice_in_dim(value_acc, value_old + value_term.reshape(key_span, kv_width), first_row, 0)
        return (key_acc, value_acc), (out_rounded.reshape(block_rows, -1), query_rows.reshape(block_rows, -1))

    empty_acc = jnp.zeros((total_rows + WINDOW, kv_width), jnp.float32)
    (key_acc, value_acc), (out_blocks, query_blocks) = lax.scan(step, (empty_acc, empty_acc), jnp.arange(total_rows // block_rows, dtype=jnp.int32))
    attended = out_blocks.reshape(total_rows, -1)
    query_grad = query_blocks.reshape(total_rows, -1)
    key_grad = key_acc[WINDOW:].astype(jnp.bfloat16)
    value_grad = value_acc[WINDOW:].astype(jnp.bfloat16)
    return (attended, query_grad, key_grad, value_grad)
```

```python
import functools
import math

import jax
import jax.numpy as jnp
from jax import lax
from jax.experimental import pallas as pl
from jax.experimental.pallas import tpu as pltpu
from jax.sharding import PartitionSpec as P


HEAD = 128
WINDOW = 1536
BLOCK = 256
SLOTS = 4
OFFSETS = (0, 2, 4, 6, 1, 3, 5)
CHUNKS = len(OFFSETS)
DOC_ROWS = 16
SCALE = HEAD ** (-0.5)
EXP2_SCALE = SCALE * math.log2(math.e)
MASKED = -1e30
NT = (((1,), (1,)), ((), ()))
VMEM = pl.BlockSpec(memory_space=pltpu.VMEM)


def dot(a, b, dims=(((1,), (0,)), ((), ()))):
    return lax.dot_general(a, b, dims, preferred_element_type=jnp.float32)


def pack_body(width, parts, a_ref, b_ref, o_ref):
    per = width // HEAD // parts
    for part in range(parts):
        for h in range(per):
            source = slice((part * per + h) * HEAD, (part * per + h + 1) * HEAD)
            o_ref[part, :, 2 * h * HEAD : (2 * h + 1) * HEAD] = a_ref[:, source]
            o_ref[part, :, (2 * h + 1) * HEAD : (2 * h + 2) * HEAD] = b_ref[:, source]


def pack(a, b, parts):
    rows, width = a.shape
    return pl.pallas_call(
        functools.partial(pack_body, width, parts),
        out_shape=jax.ShapeDtypeStruct((parts, rows, 2 * width // parts), a.dtype),
        in_specs=[VMEM, VMEM],
        out_specs=VMEM,
        compiler_params=pltpu.CompilerParams(vmem_limit_bytes=8 * 1024 * 1024),
        cost_estimate=pl.CostEstimate(flops=rows * width, bytes_accessed=8 * rows * width, transcendentals=0),
    )(a, b)


def unpack_body(width, parts, i_ref, a_ref, b_ref):
    per = width // HEAD // parts
    for part in range(parts):
        for h in range(per):
            target = slice((part * per + h) * HEAD, (part * per + h + 1) * HEAD)
            a_ref[:, target] = i_ref[part, :, 2 * h * HEAD : (2 * h + 1) * HEAD]
            b_ref[:, target] = i_ref[part, :, (2 * h + 1) * HEAD : (2 * h + 2) * HEAD]


def unpack(both):
    parts, rows, columns = both.shape
    width = parts * columns // 2
    out = jax.ShapeDtypeStruct((rows, width), both.dtype)
    return pl.pallas_call(
        functools.partial(unpack_body, width, parts),
        out_shape=(out, out),
        in_specs=[VMEM],
        out_specs=(VMEM, VMEM),
        compiler_params=pltpu.CompilerParams(vmem_limit_bytes=8 * 1024 * 1024),
        cost_estimate=pl.CostEstimate(flops=rows * width, bytes_accessed=8 * rows * width, transcendentals=0),
    )(both)


def prepare(core, own, two, four, six, mate, k_s, v_s, kt_s, vt_s, bias_s, dk_s, dv_s):
    first = 1 - core
    docs = []
    for c in range(CHUNKS):
        if c < SLOTS:
            ref = (own, two, four, six)[c]
            rows, doc = ref[:BLOCK, :], ref[BLOCK:, :]
        else:
            slot = first + (c - SLOTS)
            rows, doc = mate[slot, :BLOCK, :], mate[slot, BLOCK:, :]
        docs.append(doc[0:1, :].astype(jnp.float32))
        key, value = rows[:, :HEAD], rows[:, HEAD:]
        k_s[c] = key
        v_s[c] = value
        kt_s[c] = key.astype(jnp.float32).T.astype(jnp.bfloat16)
        vt_s[c] = value.astype(jnp.float32).T.astype(jnp.bfloat16)
    mine = docs[0]
    by_key = jnp.broadcast_to(mine, (BLOCK, BLOCK)).T
    row = lax.broadcasted_iota(jnp.int32, (BLOCK, BLOCK), 0)
    lane = lax.broadcasted_iota(jnp.int32, (BLOCK, BLOCK), 1)
    before = jnp.sum(jnp.where((by_key == mine) & (row < lane), 1.0, 0.0), axis=0, keepdims=True)
    opening = mine[:, 0:1]
    carried = jnp.zeros((1, 1), jnp.float32)
    for c in range(1, CHUNKS):
        carried = carried + jnp.sum(jnp.where(docs[c] == opening, 1.0, 0.0), axis=1, keepdims=True)
    before = before + jnp.where(mine == opening, carried, 0.0)
    before = jnp.minimum(before, WINDOW - 1.0).astype(jnp.int32)
    for c in range(CHUNKS):
        back = lane - row + OFFSETS[c] * BLOCK
        bias_s[c] = jnp.where((back >= 0) & (back <= before), 0.0, MASKED)
    dk_s[...] = jnp.zeros_like(dk_s)
    dv_s[...] = jnp.zeros_like(dv_s)


def attention_body(core_ref, x_ref, own, two, four, six, mate, y_ref, mine_ref, mate_ref, k_s, v_s, kt_s, vt_s, bias_s, s_s, dk_s, dv_s):
    head = pl.program_id(0)
    core = core_ref[0]

    @pl.when(head == 0)
    def _():
        prepare(core, own, two, four, six, mate, k_s, v_s, kt_s, vt_s, bias_s, dk_s, dv_s)

    query, grad = x_ref[:, :HEAD], x_ref[:, HEAD:]
    top = None
    for c in range(CHUNKS):
        s = dot(k_s[c], query, NT) + bias_s[c]
        s_s[c] = s
        most = jnp.max(s, axis=0, keepdims=True)
        top = most if top is None else jnp.maximum(top, most)
    total = None
    for c in range(CHUNKS):
        p = jnp.exp2((s_s[c] - top) * EXP2_SCALE)
        s_s[c] = p
        part = jnp.sum(p, axis=0, keepdims=True)
        total = part if total is None else total + part
    inverse = 1.0 / total
    out = None
    for c in range(CHUNKS):
        p16 = (s_s[c] * inverse).astype(jnp.bfloat16)
        term = dot(vt_s[c], p16)
        out = term if out is None else out + term
        dv_s[c] += dot(p16, grad)
    out16 = out.astype(jnp.bfloat16).astype(jnp.float32)
    y_ref[:, :HEAD] = out16.T.astype(jnp.bfloat16)
    delta = jnp.sum(grad.astype(jnp.float32).T * out16, axis=0, keepdims=True)
    dq = None
    for c in range(CHUNKS):
        dp = dot(v_s[c], grad, NT)
        ds = (s_s[c] * ((dp - delta) * inverse)).astype(jnp.bfloat16)
        term = dot(kt_s[c], ds)
        dq = term if dq is None else dq + term
        dk_s[c] += dot(ds, query)
    y_ref[:, HEAD:] = (dq * SCALE).T.astype(jnp.bfloat16)

    @pl.when(head == pl.num_programs(0) - 1)
    def _():
        for t in range(SLOTS):
            mine_ref[t, :, :HEAD] = dk_s[t] * SCALE
            mine_ref[t, :, HEAD:] = dv_s[t]
        first = 1 - core
        mate_ref[3 - 3 * first] = jnp.zeros((BLOCK, 2 * HEAD), jnp.bfloat16)
        for t in range(SLOTS - 1):
            mate_ref[first + t, :, :HEAD] = (dk_s[SLOTS + t] * SCALE).astype(jnp.bfloat16)
            mate_ref[first + t, :, HEAD:] = dv_s[SLOTS + t].astype(jnp.bfloat16)


def attention(core, x, own, two, four, six, mate):
    heads = x.shape[1] // (2 * HEAD)
    flops = heads * 6 * 2 * CHUNKS * BLOCK * BLOCK * HEAD
    whole = lambda shape: pl.BlockSpec(shape, lambda h, _: (0,) * len(shape))
    block = whole((BLOCK + DOC_ROWS, 2 * HEAD))
    return pl.pallas_call(
        attention_body,
        out_shape=(
            jax.ShapeDtypeStruct(x.shape, jnp.bfloat16),
            jax.ShapeDtypeStruct((SLOTS, BLOCK, 2 * HEAD), jnp.float32),
            jax.ShapeDtypeStruct((SLOTS, BLOCK, 2 * HEAD), jnp.bfloat16),
        ),
        grid_spec=pltpu.PrefetchScalarGridSpec(
            num_scalar_prefetch=1,
            grid=(heads,),
            in_specs=[
                pl.BlockSpec((BLOCK, 2 * HEAD), lambda h, _: (0, h)),
                block,
                block,
                block,
                block,
                whole((SLOTS, BLOCK + DOC_ROWS, 2 * HEAD)),
            ],
            out_specs=(
                pl.BlockSpec((BLOCK, 2 * HEAD), lambda h, _: (0, h)),
                whole((SLOTS, BLOCK, 2 * HEAD)),
                whole((SLOTS, BLOCK, 2 * HEAD)),
            ),
            scratch_shapes=[
                pltpu.VMEM((CHUNKS, BLOCK, HEAD), jnp.bfloat16),
                pltpu.VMEM((CHUNKS, BLOCK, HEAD), jnp.bfloat16),
                pltpu.VMEM((CHUNKS, HEAD, BLOCK), jnp.bfloat16),
                pltpu.VMEM((CHUNKS, HEAD, BLOCK), jnp.bfloat16),
                pltpu.VMEM((CHUNKS, BLOCK, BLOCK), jnp.float32),
                pltpu.VMEM((CHUNKS, BLOCK, BLOCK), jnp.float32),
                pltpu.VMEM((CHUNKS, BLOCK, HEAD), jnp.float32),
                pltpu.VMEM((CHUNKS, BLOCK, HEAD), jnp.float32),
            ],
        ),
        compiler_params=pltpu.CompilerParams(dimension_semantics=("arbitrary",), vmem_limit_bytes=20 * 1024 * 1024),
        cost_estimate=pl.CostEstimate(flops=flops, bytes_accessed=5 * 1024 * 1024, transcendentals=heads * CHUNKS * BLOCK * BLOCK),
        name="attention",
    )(core, x, own, two, four, six, mate)


def shift(value, steps):
    count = lax.axis_size("ctx")
    return lax.ppermute(value, "ctx", [(s, s + steps) for s in range(max(0, -steps), min(count, count - steps))])


def swap(value):
    count = lax.axis_size("ctx")
    return lax.ppermute(value, "ctx", [(s, s ^ 1) for s in range(count)])


def over_head(value):
    return lax.all_to_all(value, "head", split_axis=0, concat_axis=0, tiled=True)


def local(queries, key_heads, value_head_array, out_grad, doc_ids):
    parts = lax.axis_size("head")
    core = (lax.axis_index("ctx") % 2).astype(jnp.int32).reshape(1)
    kv = over_head(pack(key_heads, value_head_array, parts))
    kv = kv.reshape(BLOCK, 2 * HEAD)
    docs = jnp.pad((doc_ids + 1).astype(jnp.bfloat16)[None, :], ((0, DOC_ROWS - 1), (0, 0)))
    own = jnp.concatenate([kv, docs], axis=0)
    packed = pack(queries, out_grad, parts)
    x = over_head(packed).reshape(BLOCK, -1)
    two, four, six = (shift(own, steps) for steps in (2, 4, 6))
    mate = swap(jnp.stack([own, two, four, six]))
    y, mine, sent = attention(core, x, own, two, four, six, mate)
    y = over_head(y.reshape(parts, -1, y.shape[1]))
    sent = swap(sent)
    sums = mine + sent.astype(jnp.float32)
    rounded = sums.astype(jnp.bfloat16)
    back = [shift(rounded[t], -2 * t) for t in range(1, SLOTS)]
    grads = sums[0] + sum(b.astype(jnp.float32) for b in back)
    grads = grads.astype(jnp.bfloat16)
    grads = over_head(grads.reshape(parts, -1, 2 * HEAD))
    attended, query_grad = unpack(y)
    key_grad, value_grad = unpack(grads)
    return attended, query_grad, key_grad, value_grad


def solution(mesh):
    rows = P(("ctx", "head"), None)

    return jax.shard_map(
        local,
        mesh=mesh,
        in_specs=(rows, rows, rows, rows, P("ctx")),
        out_specs=(rows, rows, rows, rows),
        check_vma=False,
    )
```

```python
import functools
import math

import jax
import jax.numpy as jnp
from jax import lax
from jax.experimental import pallas as pl
from jax.experimental.pallas import tpu as pltpu
from jax.sharding import PartitionSpec as P


HEAD = 128
WINDOW = 1536
BLOCK = 256
SLOTS = 4
OFFSETS = (0, 2, 4, 6, 1, 3, 5)
CHUNKS = len(OFFSETS)
DOC_ROWS = 16
SCALE = HEAD ** (-0.5)
EXP2_SCALE = SCALE * math.log2(math.e)
MASKED = -1e30
NT = (((1,), (1,)), ((), ()))
VMEM = pl.BlockSpec(memory_space=pltpu.VMEM)
SMEM = pl.BlockSpec(memory_space=pltpu.SMEM)
SMALL = pltpu.CompilerParams(vmem_limit_bytes=8 * 1024 * 1024)


def dot(a, b, dims=(((1,), (0,)), ((), ()))):
    return lax.dot_general(a, b, dims, preferred_element_type=jnp.float32)


def pack_body(width, parts, a_ref, b_ref, o_ref):
    per = width // HEAD // parts
    for part in range(parts):
        for h in range(per):
            source = slice((part * per + h) * HEAD, (part * per + h + 1) * HEAD)
            o_ref[part, :, 2 * h * HEAD : (2 * h + 1) * HEAD] = a_ref[:, source]
            o_ref[part, :, (2 * h + 1) * HEAD : (2 * h + 2) * HEAD] = b_ref[:, source]


def pack(a, b, parts):
    rows, width = a.shape
    return pl.pallas_call(
        functools.partial(pack_body, width, parts),
        out_shape=jax.ShapeDtypeStruct((parts, rows, 2 * width // parts), a.dtype),
        in_specs=[VMEM, VMEM],
        out_specs=VMEM,
        compiler_params=SMALL,
        cost_estimate=pl.CostEstimate(flops=rows * width, bytes_accessed=8 * rows * width, transcendentals=0),
    )(a, b)


def cut_body(parts, at_ref, a_ref, b_ref, *o_refs):
    for k in range(parts):
        source = pl.ds(pl.multiple_of(lax.rem(at_ref[0] + k, parts) * HEAD, HEAD), HEAD)
        o_refs[k][:, :HEAD] = a_ref[:, source]
        o_refs[k][:, HEAD:] = b_ref[:, source]


def cut(at, a, b, parts):
    rows = a.shape[0]
    piece = jax.ShapeDtypeStruct((rows, 2 * HEAD), a.dtype)
    return pl.pallas_call(
        functools.partial(cut_body, parts),
        out_shape=(piece,) * parts,
        in_specs=[SMEM, VMEM, VMEM],
        out_specs=(VMEM,) * parts,
        compiler_params=SMALL,
        cost_estimate=pl.CostEstimate(flops=a.size, bytes_accessed=8 * a.size, transcendentals=0),
        name="cut",
    )(at, a, b)


def assemble_body(parts, at_ref, doc_ref, *refs):
    o_ref = refs[parts]
    rows = refs[0].shape[0]
    for k in range(parts):
        target = pl.multiple_of(lax.rem(at_ref[0] + (parts - k), parts) * rows, rows)
        o_ref[pl.ds(target, rows), :] = refs[k][...]
    doc = (doc_ref[...] + 1).astype(jnp.float32)
    o_ref[parts * rows :, :] = jnp.broadcast_to(doc, (DOC_ROWS, parts * rows)).astype(jnp.bfloat16)


def assemble(at, docs, pieces):
    parts, (rows, columns) = len(pieces), pieces[0].shape
    return pl.pallas_call(
        functools.partial(assemble_body, parts),
        out_shape=jax.ShapeDtypeStruct((parts * rows + DOC_ROWS, columns), pieces[0].dtype),
        in_specs=[SMEM] + [VMEM] * (parts + 1),
        out_specs=VMEM,
        compiler_params=SMALL,
        cost_estimate=pl.CostEstimate(flops=parts * rows * columns, bytes_accessed=4 * parts * rows * columns, transcendentals=0),
        name="assemble",
    )(at, docs[None, :], *pieces)


def add_cut_body(parts, at_ref, base_ref, one_ref, two_ref, three_ref, *o_refs):
    rows = o_refs[0].shape[0]
    for k in range(parts):
        source = pl.ds(pl.multiple_of(lax.rem(at_ref[0] + k, parts) * rows, rows), rows)
        total = base_ref[source, :] + one_ref[source, :].astype(jnp.float32)
        total = total + two_ref[source, :].astype(jnp.float32) + three_ref[source, :].astype(jnp.float32)
        o_refs[k][...] = total.astype(jnp.bfloat16)


def add_cut(at, base, others, parts):
    rows, columns = base.shape[0] // parts, base.shape[1]
    piece = jax.ShapeDtypeStruct((rows, columns), jnp.bfloat16)
    return pl.pallas_call(
        functools.partial(add_cut_body, parts),
        out_shape=(piece,) * parts,
        in_specs=[SMEM] + [VMEM] * 4,
        out_specs=(VMEM,) * parts,
        compiler_params=SMALL,
        cost_estimate=pl.CostEstimate(flops=4 * base.size, bytes_accessed=12 * base.size, transcendentals=0),
        name="add_cut",
    )(at, base, *others)


def join_body(parts, at_ref, *refs):
    a_ref, b_ref = refs[parts:]
    for k in range(parts):
        target = pl.ds(pl.multiple_of(lax.rem(at_ref[0] + (parts - k), parts) * HEAD, HEAD), HEAD)
        a_ref[:, target] = refs[k][:, :HEAD]
        b_ref[:, target] = refs[k][:, HEAD:]


def join(at, pieces):
    parts, rows = len(pieces), pieces[0].shape[0]
    out = jax.ShapeDtypeStruct((rows, parts * HEAD), pieces[0].dtype)
    return pl.pallas_call(
        functools.partial(join_body, parts),
        out_shape=(out, out),
        in_specs=[SMEM] + [VMEM] * parts,
        out_specs=(VMEM, VMEM),
        compiler_params=SMALL,
        cost_estimate=pl.CostEstimate(flops=out.size, bytes_accessed=8 * out.size, transcendentals=0),
        name="join",
    )(at, *pieces)


def unpack_body(width, parts, i_ref, a_ref, b_ref):
    per = width // HEAD // parts
    for part in range(parts):
        for h in range(per):
            target = slice((part * per + h) * HEAD, (part * per + h + 1) * HEAD)
            a_ref[:, target] = i_ref[part, :, 2 * h * HEAD : (2 * h + 1) * HEAD]
            b_ref[:, target] = i_ref[part, :, (2 * h + 1) * HEAD : (2 * h + 2) * HEAD]


def unpack(both):
    parts, rows, columns = both.shape
    width = parts * columns // 2
    out = jax.ShapeDtypeStruct((rows, width), both.dtype)
    return pl.pallas_call(
        functools.partial(unpack_body, width, parts),
        out_shape=(out, out),
        in_specs=[VMEM],
        out_specs=(VMEM, VMEM),
        compiler_params=SMALL,
        cost_estimate=pl.CostEstimate(flops=rows * width, bytes_accessed=8 * rows * width, transcendentals=0),
    )(both)


def prepare(core, own, two, four, six, mate, k_s, v_s, kt_s, vt_s, bias_s, dk_s, dv_s):
    first = 1 - core
    docs = []
    for c in range(CHUNKS):
        if c < SLOTS:
            ref = (own, two, four, six)[c]
            rows, doc = ref[:BLOCK, :], ref[BLOCK:, :]
        else:
            slot = first + (c - SLOTS)
            rows, doc = mate[slot, :BLOCK, :], mate[slot, BLOCK:, :]
        docs.append(doc[0:1, :].astype(jnp.float32))
        key, value = rows[:, :HEAD], rows[:, HEAD:]
        k_s[c] = key
        v_s[c] = value
        kt_s[c] = key.astype(jnp.float32).T.astype(jnp.bfloat16)
        vt_s[c] = value.astype(jnp.float32).T.astype(jnp.bfloat16)
    mine = docs[0]
    by_key = jnp.broadcast_to(mine, (BLOCK, BLOCK)).T
    row = lax.broadcasted_iota(jnp.int32, (BLOCK, BLOCK), 0)
    lane = lax.broadcasted_iota(jnp.int32, (BLOCK, BLOCK), 1)
    before = jnp.sum(jnp.where((by_key == mine) & (row < lane), 1.0, 0.0), axis=0, keepdims=True)
    opening = mine[:, 0:1]
    carried = jnp.zeros((1, 1), jnp.float32)
    for c in range(1, CHUNKS):
        carried = carried + jnp.sum(jnp.where(docs[c] == opening, 1.0, 0.0), axis=1, keepdims=True)
    before = before + jnp.where(mine == opening, carried, 0.0)
    before = jnp.minimum(before, WINDOW - 1.0).astype(jnp.int32)
    for c in range(CHUNKS):
        back = lane - row + OFFSETS[c] * BLOCK
        bias_s[c] = jnp.where((back >= 0) & (back <= before), 0.0, MASKED)
    dk_s[...] = jnp.zeros_like(dk_s)
    dv_s[...] = jnp.zeros_like(dv_s)


def attention_body(core_ref, x_ref, own, two, four, six, mate, y_ref, mine_ref, mate_ref, k_s, v_s, kt_s, vt_s, bias_s, s_s, dk_s, dv_s):
    head = pl.program_id(0)
    core = core_ref[0]

    @pl.when(head == 0)
    def _():
        prepare(core, own, two, four, six, mate, k_s, v_s, kt_s, vt_s, bias_s, dk_s, dv_s)

    query, grad = x_ref[:, :HEAD], x_ref[:, HEAD:]
    top = None
    for c in range(CHUNKS):
        s = dot(k_s[c], query, NT) + bias_s[c]
        s_s[c] = s
        most = jnp.max(s, axis=0, keepdims=True)
        top = most if top is None else jnp.maximum(top, most)
    total = None
    for c in range(CHUNKS):
        p = jnp.exp2((s_s[c] - top) * EXP2_SCALE)
        s_s[c] = p
        part = jnp.sum(p, axis=0, keepdims=True)
        total = part if total is None else total + part
    inverse = 1.0 / total
    out = None
    for c in range(CHUNKS):
        p16 = (s_s[c] * inverse).astype(jnp.bfloat16)
        term = dot(vt_s[c], p16)
        out = term if out is None else out + term
        dv_s[c] += dot(p16, grad)
    out16 = out.astype(jnp.bfloat16).astype(jnp.float32)
    y_ref[:, :HEAD] = out16.T.astype(jnp.bfloat16)
    delta = jnp.sum(grad.astype(jnp.float32).T * out16, axis=0, keepdims=True)
    dq = None
    for c in range(CHUNKS):
        dp = dot(v_s[c], grad, NT)
        ds = (s_s[c] * ((dp - delta) * inverse)).astype(jnp.bfloat16)
        term = dot(kt_s[c], ds)
        dq = term if dq is None else dq + term
        dk_s[c] += dot(ds, query)
    y_ref[:, HEAD:] = (dq * SCALE).T.astype(jnp.bfloat16)

    @pl.when(head == pl.num_programs(0) - 1)
    def _():
        for t in range(SLOTS):
            mine_ref[t, :, :HEAD] = dk_s[t] * SCALE
            mine_ref[t, :, HEAD:] = dv_s[t]
        first = 1 - core
        mate_ref[3 - 3 * first] = jnp.zeros((BLOCK, 2 * HEAD), jnp.bfloat16)
        for t in range(SLOTS - 1):
            mate_ref[first + t, :, :HEAD] = (dk_s[SLOTS + t] * SCALE).astype(jnp.bfloat16)
            mate_ref[first + t, :, HEAD:] = dv_s[SLOTS + t].astype(jnp.bfloat16)


def attention(core, x, own, two, four, six, mate):
    heads = x.shape[1] // (2 * HEAD)
    flops = heads * 6 * 2 * CHUNKS * BLOCK * BLOCK * HEAD
    whole = lambda shape: pl.BlockSpec(shape, lambda h, _: (0,) * len(shape))
    block = whole((BLOCK + DOC_ROWS, 2 * HEAD))
    return pl.pallas_call(
        attention_body,
        out_shape=(
            jax.ShapeDtypeStruct(x.shape, jnp.bfloat16),
            jax.ShapeDtypeStruct((SLOTS, BLOCK, 2 * HEAD), jnp.float32),
            jax.ShapeDtypeStruct((SLOTS, BLOCK, 2 * HEAD), jnp.bfloat16),
        ),
        grid_spec=pltpu.PrefetchScalarGridSpec(
            num_scalar_prefetch=1,
            grid=(heads,),
            in_specs=[
                pl.BlockSpec((BLOCK, 2 * HEAD), lambda h, _: (0, h)),
                block,
                block,
                block,
                block,
                whole((SLOTS, BLOCK + DOC_ROWS, 2 * HEAD)),
            ],
            out_specs=(
                pl.BlockSpec((BLOCK, 2 * HEAD), lambda h, _: (0, h)),
                whole((SLOTS, BLOCK, 2 * HEAD)),
                whole((SLOTS, BLOCK, 2 * HEAD)),
            ),
            scratch_shapes=[
                pltpu.VMEM((CHUNKS, BLOCK, HEAD), jnp.bfloat16),
                pltpu.VMEM((CHUNKS, BLOCK, HEAD), jnp.bfloat16),
                pltpu.VMEM((CHUNKS, HEAD, BLOCK), jnp.bfloat16),
                pltpu.VMEM((CHUNKS, HEAD, BLOCK), jnp.bfloat16),
                pltpu.VMEM((CHUNKS, BLOCK, BLOCK), jnp.float32),
                pltpu.VMEM((CHUNKS, BLOCK, BLOCK), jnp.float32),
                pltpu.VMEM((CHUNKS, BLOCK, HEAD), jnp.float32),
                pltpu.VMEM((CHUNKS, BLOCK, HEAD), jnp.float32),
            ],
        ),
        compiler_params=pltpu.CompilerParams(dimension_semantics=("arbitrary",), vmem_limit_bytes=20 * 1024 * 1024),
        cost_estimate=pl.CostEstimate(flops=flops, bytes_accessed=5 * 1024 * 1024, transcendentals=heads * CHUNKS * BLOCK * BLOCK),
        name="attention",
    )(core, x, own, two, four, six, mate)


def shift(value, steps):
    count = lax.axis_size("ctx")
    return lax.ppermute(value, "ctx", [(s, s + steps) for s in range(max(0, -steps), min(count, count - steps))])


def swap(value):
    count = lax.axis_size("ctx")
    return lax.ppermute(value, "ctx", [(s, s ^ 1) for s in range(count)])


def over_head(value):
    return lax.all_to_all(value, "head", split_axis=0, concat_axis=0, tiled=True)


def around(value, steps):
    count = lax.axis_size("head")
    return lax.ppermute(value, "head", [(s, (s + steps) % count) for s in range(count)])


def exchange(pieces):
    return [pieces[0]] + [around(piece, k) for k, piece in enumerate(pieces) if k]


def local(queries, key_heads, value_head_array, out_grad, doc_ids):
    parts = lax.axis_size("head")
    core = (lax.axis_index("ctx") % 2).astype(jnp.int32).reshape(1)
    at = lax.axis_index("head").astype(jnp.int32).reshape(1)
    pieces = cut(at, key_heads, value_head_array, parts)
    packed = pack(queries, out_grad, parts)
    x = over_head(packed).reshape(BLOCK, -1)
    pieces = exchange(pieces)
    own = assemble(at, doc_ids, pieces)
    two, four, six = (shift(own, steps) for steps in (2, 4, 6))
    mate = swap(jnp.stack([own, two, four, six]))
    y, mine, sent = attention(core, x, own, two, four, six, mate)
    y = over_head(y.reshape(parts, -1, y.shape[1]))
    sent = swap(sent)
    sums = mine + sent.astype(jnp.float32)
    rounded = sums.astype(jnp.bfloat16)
    back = [shift(rounded[t], -2 * t) for t in range(1, SLOTS)]
    pieces = add_cut(at, sums[0], back, parts)
    pieces = exchange(pieces)
    attended, query_grad = unpack(y)
    key_grad, value_grad = join(at, pieces)
    return attended, query_grad, key_grad, value_grad


def solution(mesh):
    rows = P(("ctx", "head"), None)

    return jax.shard_map(
        local,
        mesh=mesh,
        in_specs=(rows, rows, rows, rows, P("ctx")),
        out_specs=(rows, rows, rows, rows),
        check_vma=False,
    )
```

```python
import functools
import math

import jax
import jax.numpy as jnp
from jax import lax
from jax.experimental import pallas as pl
from jax.experimental.pallas import tpu as pltpu
from jax.sharding import PartitionSpec as P


HEAD = 128
WINDOW = 1536
BLOCK = 256
SLOTS = 4
OFFSETS = (0, 2, 4, 6, 1, 3, 5)
CHUNKS = len(OFFSETS)
DOC_ROWS = 16
PIECE = 64
SCALE = HEAD ** (-0.5)
EXP2_SCALE = SCALE * math.log2(math.e)
MASKED = -1e30
NT = (((1,), (1,)), ((), ()))
VMEM = pl.BlockSpec(memory_space=pltpu.VMEM)
SMALL = pltpu.CompilerParams(vmem_limit_bytes=8 * 1024 * 1024)


def dot(a, b, dims=(((1,), (0,)), ((), ()))):
    return lax.dot_general(a, b, dims, preferred_element_type=jnp.float32)


def run(copies):
    for copy in copies:
        copy.start()
    for copy in copies:
        copy.wait()


def pack_body(parts, *refs):
    ins, o_ref, sems = refs[:-2], refs[-2], refs[-1]
    copies = []
    for part in range(parts):
        start = 0
        for ref in ins:
            width = ref.shape[1] // parts
            source, target = ref.at[:, pl.ds(part * width, width)], o_ref.at[part, :, pl.ds(start, width)]
            copies.append(pltpu.make_async_copy(source, target, sems.at[len(copies)]))
            start += width
    run(copies)


def pack(arrays, parts):
    rows, width = arrays[0].shape[0], sum(a.shape[1] for a in arrays)
    return pl.pallas_call(
        functools.partial(pack_body, parts),
        out_shape=jax.ShapeDtypeStruct((parts, rows, width // parts), arrays[0].dtype),
        in_specs=[pl.BlockSpec(memory_space=pl.ANY)] * len(arrays),
        out_specs=VMEM,
        scratch_shapes=[pltpu.SemaphoreType.DMA((parts * len(arrays),))],
        cost_estimate=pl.CostEstimate(flops=rows * width, bytes_accessed=4 * rows * width, transcendentals=0),
    )(*arrays)


def unpack_body(parts, i_ref, *refs):
    outs, sems = refs[:-1], refs[-1]
    copies = []
    for part in range(parts):
        start = 0
        for ref in outs:
            width = ref.shape[1] // parts
            source, target = i_ref.at[part, :, pl.ds(start, width)], ref.at[:, pl.ds(part * width, width)]
            copies.append(pltpu.make_async_copy(source, target, sems.at[len(copies)]))
            start += width
    run(copies)


def unpack(value, widths):
    parts, rows, _ = value.shape
    return pl.pallas_call(
        functools.partial(unpack_body, parts),
        out_shape=tuple(jax.ShapeDtypeStruct((rows, parts * width), value.dtype) for width in widths),
        in_specs=[VMEM],
        out_specs=(pl.BlockSpec(memory_space=pl.ANY),) * len(widths),
        scratch_shapes=[pltpu.SemaphoreType.DMA((parts * len(widths),))],
        compiler_params=SMALL,
        cost_estimate=pl.CostEstimate(flops=value.size, bytes_accessed=4 * value.size, transcendentals=0),
    )(value)


def add_body(dq_ref, base_ref, one_ref, two_ref, three_ref, o_ref):
    width = dq_ref.shape[1]
    o_ref[:, :width] = dq_ref[...]
    total = base_ref[...] + one_ref[...].astype(jnp.float32)
    total = total + two_ref[...].astype(jnp.float32) + three_ref[...].astype(jnp.float32)
    o_ref[:, width:] = total.astype(jnp.bfloat16)


def add(dq, base, others):
    rows, width = dq.shape[0], dq.shape[1] + base.shape[1]
    return pl.pallas_call(
        add_body,
        out_shape=jax.ShapeDtypeStruct((rows, width), jnp.bfloat16),
        in_specs=[VMEM] * 5,
        out_specs=VMEM,
        compiler_params=SMALL,
        cost_estimate=pl.CostEstimate(flops=4 * base.size, bytes_accessed=4 * rows * width, transcendentals=0),
        name="add",
    )(dq, base, *others)


def prepare(core, own, two, four, six, mate, k_s, v_s, kt_s, vt_s, bias_s, dk_s, dv_s):
    first = 1 - core
    docs = []
    for c in range(CHUNKS):
        if c < SLOTS:
            ref = (own, two, four, six)[c]
            rows, doc = ref[:BLOCK, :], ref[BLOCK:, :]
        else:
            slot = first + (c - SLOTS)
            rows, doc = mate[slot, :BLOCK, :], mate[slot, BLOCK:, :]
        docs.append(doc[0:1, :].astype(jnp.float32))
        key, value = rows[:, :HEAD], rows[:, HEAD:]
        k_s[c] = key
        v_s[c] = value
        kt_s[c] = key.astype(jnp.float32).T.astype(jnp.bfloat16)
        vt_s[c] = value.astype(jnp.float32).T.astype(jnp.bfloat16)
    mine = docs[0]
    by_key = jnp.broadcast_to(mine, (BLOCK, BLOCK)).T
    row = lax.broadcasted_iota(jnp.int32, (BLOCK, BLOCK), 0)
    lane = lax.broadcasted_iota(jnp.int32, (BLOCK, BLOCK), 1)
    before = jnp.sum(jnp.where((by_key == mine) & (row < lane), 1.0, 0.0), axis=0, keepdims=True)
    opening = mine[:, 0:1]
    carried = jnp.zeros((1, 1), jnp.float32)
    for c in range(1, CHUNKS):
        carried = carried + jnp.sum(jnp.where(docs[c] == opening, 1.0, 0.0), axis=1, keepdims=True)
    before = before + jnp.where(mine == opening, carried, 0.0)
    before = jnp.minimum(before, WINDOW - 1.0).astype(jnp.int32)
    for c in range(CHUNKS):
        back = lane - row + OFFSETS[c] * BLOCK
        bias_s[c] = jnp.where((back >= 0) & (back <= before), 0.0, MASKED)
    dk_s[...] = jnp.zeros_like(dk_s)
    dv_s[...] = jnp.zeros_like(dv_s)


def scores(query, s_ref, k_s, bias_s):
    top = None
    for c in range(CHUNKS):
        s = dot(k_s[c], query, NT) * EXP2_SCALE + bias_s[c]
        s_ref[c] = s
        most = jnp.max(s, axis=0, keepdims=True)
        top = most if top is None else jnp.maximum(top, most)
    return top


def weigh(c, s_ref, top, total):
    for r in range(0, BLOCK, PIECE):
        p = jnp.exp2(s_ref[c, r : r + PIECE, :] - top)
        s_ref[c, r : r + PIECE, :] = p
        part = jnp.sum(p, axis=0, keepdims=True)
        total = part if total is None else total + part
    return total


def collect(grad, s_ref, total, att_ref, columns, stat_ref, vt_s, dv_s):
    inverse = 1.0 / total
    out = None
    for c in range(CHUNKS):
        p16 = (s_ref[c] * inverse).astype(jnp.bfloat16)
        term = dot(vt_s[c], p16)
        out = term if out is None else out + term
        dv_s[c] += dot(p16, grad)
    out16 = out.astype(jnp.bfloat16).astype(jnp.float32)
    att_ref[:, columns] = out16.T.astype(jnp.bfloat16)
    delta = jnp.sum(grad.astype(jnp.float32).T * out16, axis=0, keepdims=True)
    stat_ref[0:1, :] = inverse
    stat_ref[1:2, :] = delta


def step(ahead, behind, q_ref, g_ref, att_ref, dq_ref, k_s, v_s, kt_s, vt_s, bias_s, dk_s, dv_s):
    columns = lambda head: pl.ds(pl.multiple_of(head * HEAD, HEAD), HEAD)
    total = dq = None
    if ahead:
        head, s_ref, stat_ref = ahead
        grad = g_ref[:, columns(head)]
        top = scores(q_ref[:, columns(head)], s_ref, k_s, bias_s)
    if behind:
        last, p_ref, last_ref = behind
        last_query, last_grad = q_ref[:, columns(last)], g_ref[:, columns(last)]
        inverse, delta = last_ref[0:1, :], last_ref[1:2, :]
        coming = dot(v_s[0], last_grad, NT)
    for c in range(CHUNKS):
        if behind:
            dp = coming
            if c + 1 < CHUNKS:
                coming = dot(v_s[c + 1], last_grad, NT)
        if ahead:
            total = weigh(c, s_ref, top, total)
        if behind:
            ds = (p_ref[c] * ((dp - delta) * inverse)).astype(jnp.bfloat16)
            term = dot(kt_s[c], ds)
            dq = term if dq is None else dq + term
            dk_s[c] += dot(ds, last_query)
    if behind:
        dq_ref[:, columns(last)] = (dq * SCALE).T.astype(jnp.bfloat16)
    if ahead:
        collect(grad, s_ref, total, att_ref, columns(head), stat_ref, vt_s, dv_s)


def attention_body(core_ref, q_ref, g_ref, own, two, four, six, mate, att_ref, dq_ref, mine_ref, mate_ref, k_s, v_s, kt_s, vt_s, bias_s, dk_s, dv_s, even_s, odd_s, even_t, odd_t):
    core = core_ref[0]
    heads = dq_ref.shape[1] // HEAD
    prepare(core, own, two, four, six, mate, k_s, v_s, kt_s, vt_s, bias_s, dk_s, dv_s)
    refs = (q_ref, g_ref, att_ref, dq_ref, k_s, v_s, kt_s, vt_s, bias_s, dk_s, dv_s)
    step((0, even_s, even_t), None, *refs)

    def pair(i, _):
        head = 2 * i
        step((head + 1, odd_s, odd_t), (head, even_s, even_t), *refs)
        step((head + 2, even_s, even_t), (head + 1, odd_s, odd_t), *refs)
        return 0

    lax.fori_loop(0, heads // 2 - 1, pair, 0)
    step((heads - 1, odd_s, odd_t), (heads - 2, even_s, even_t), *refs)
    step(None, (heads - 1, odd_s, odd_t), *refs)
    for t in range(SLOTS):
        mine_ref[t, :, :HEAD] = dk_s[t] * SCALE
        mine_ref[t, :, HEAD:] = dv_s[t]
    first = 1 - core
    mate_ref[3 - 3 * first] = jnp.zeros((BLOCK, 2 * HEAD), jnp.bfloat16)
    for t in range(SLOTS - 1):
        mate_ref[first + t, :, :HEAD] = (dk_s[SLOTS + t] * SCALE).astype(jnp.bfloat16)
        mate_ref[first + t, :, HEAD:] = dv_s[SLOTS + t].astype(jnp.bfloat16)


def attention(core, q, g, own, two, four, six, mate):
    heads = g.shape[1] // HEAD
    work = heads * CHUNKS * BLOCK * BLOCK
    scratch = lambda dims, kind: pltpu.VMEM(dims, kind)
    return pl.pallas_call(
        attention_body,
        out_shape=(
            jax.ShapeDtypeStruct(g.shape, jnp.bfloat16),
            jax.ShapeDtypeStruct(g.shape, jnp.bfloat16),
            jax.ShapeDtypeStruct((SLOTS, BLOCK, 2 * HEAD), jnp.float32),
            jax.ShapeDtypeStruct((SLOTS, BLOCK, 2 * HEAD), jnp.bfloat16),
        ),
        in_specs=[pl.BlockSpec(memory_space=pltpu.SMEM)] + [VMEM] * 7,
        out_specs=(VMEM,) * 4,
        scratch_shapes=[
            scratch((CHUNKS, BLOCK, HEAD), jnp.bfloat16),
            scratch((CHUNKS, BLOCK, HEAD), jnp.bfloat16),
            scratch((CHUNKS, HEAD, BLOCK), jnp.bfloat16),
            scratch((CHUNKS, HEAD, BLOCK), jnp.bfloat16),
            scratch((CHUNKS, BLOCK, BLOCK), jnp.float32),
            scratch((CHUNKS, BLOCK, HEAD), jnp.float32),
            scratch((CHUNKS, BLOCK, HEAD), jnp.float32),
            scratch((CHUNKS, BLOCK, BLOCK), jnp.float32),
            scratch((CHUNKS, BLOCK, BLOCK), jnp.float32),
            scratch((8, BLOCK), jnp.float32),
            scratch((8, BLOCK), jnp.float32),
        ],
        compiler_params=pltpu.CompilerParams(vmem_limit_bytes=16 * 1024 * 1024),
        cost_estimate=pl.CostEstimate(flops=12 * work * HEAD, bytes_accessed=5 * 1024 * 1024, transcendentals=work),
        name="attention",
    )(core, q, g, own, two, four, six, mate)


def shift(value, steps):
    count = lax.axis_size("ctx")
    return lax.ppermute(value, "ctx", [(s, s + steps) for s in range(max(0, -steps), min(count, count - steps))])


def swap(value):
    count = lax.axis_size("ctx")
    return lax.ppermute(value, "ctx", [(s, s ^ 1) for s in range(count)])


def over_head(value):
    return lax.all_to_all(value, "head", split_axis=0, concat_axis=0, tiled=True)


def local(queries, key_heads, value_head_array, out_grad, doc_ids):
    parts = lax.axis_size("head")
    core = (lax.axis_index("ctx") % 2).astype(jnp.int32).reshape(1)
    q = over_head(pack((queries, key_heads, value_head_array), parts)).reshape(BLOCK, -1)
    packed = pack((out_grad,), parts)
    g = over_head(packed).reshape(BLOCK, -1)
    docs = jnp.pad((doc_ids + 1).astype(jnp.bfloat16)[None, :], ((0, DOC_ROWS - 1), (0, 0)))
    own = jnp.concatenate([q[:, -2 * HEAD :], docs], axis=0)
    two, four, six = (shift(own, steps) for steps in (2, 4, 6))
    mate = swap(jnp.stack([own, two, four, six]))
    attended, dq, mine, sent = attention(core, q, g, own, two, four, six, mate)
    attended = over_head(attended.reshape(parts, -1, attended.shape[1]))
    sent = swap(sent)
    sums = mine + sent.astype(jnp.float32)
    rounded = sums.astype(jnp.bfloat16)
    back = [shift(rounded[t], -2 * t) for t in range(1, SLOTS)]
    grads = add(dq, sums[0], back)
    grads = over_head(grads.reshape(parts, -1, grads.shape[1]))
    (attended,) = unpack(attended, (attended.shape[2],))
    query_grad, key_grad, value_grad = unpack(grads, (dq.shape[1], HEAD, HEAD))
    return attended, query_grad, key_grad, value_grad


def solution(mesh):
    rows = P(("ctx", "head"), None)

    return jax.shard_map(
        local,
        mesh=mesh,
        in_specs=(rows, rows, rows, rows, P("ctx")),
        out_specs=(rows, rows, rows, rows),
        check_vma=False,
    )
```

```python
import functools
import math

import jax
import jax.numpy as jnp
from jax import lax
from jax.experimental import pallas as pl
from jax.experimental.pallas import tpu as pltpu
from jax.sharding import PartitionSpec as P


HEAD = 128
WINDOW = 1536
BLOCK = 256
SLOTS = 4
OFFSETS = (0, 2, 4, 6, 1, 3, 5)
CHUNKS = len(OFFSETS)
DOC_ROWS = 16
PIECE = 64
SCALE = HEAD ** (-0.5)
EXP2_SCALE = SCALE * math.log2(math.e)
MASKED = -1e30
NT = (((1,), (1,)), ((), ()))
VMEM = pl.BlockSpec(memory_space=pltpu.VMEM)
SMEM = pl.BlockSpec(memory_space=pltpu.SMEM)
SMALL = pltpu.CompilerParams(vmem_limit_bytes=8 * 1024 * 1024)


def dot(a, b, dims=(((1,), (0,)), ((), ()))):
    return lax.dot_general(a, b, dims, preferred_element_type=jnp.float32)


def run(copies):
    for copy in copies:
        copy.start()
    for copy in copies:
        copy.wait()


def pack_body(parts, *refs):
    ins, o_ref, sems = refs[:-2], refs[-2], refs[-1]
    copies = []
    for part in range(parts):
        start = 0
        for ref in ins:
            width = ref.shape[1] // parts
            source, target = ref.at[:, pl.ds(part * width, width)], o_ref.at[part, :, pl.ds(start, width)]
            copies.append(pltpu.make_async_copy(source, target, sems.at[len(copies)]))
            start += width
    run(copies)


def pack(arrays, parts):
    rows, width = arrays[0].shape[0], sum(a.shape[1] for a in arrays)
    return pl.pallas_call(
        functools.partial(pack_body, parts),
        out_shape=jax.ShapeDtypeStruct((parts, rows, width // parts), arrays[0].dtype),
        in_specs=[pl.BlockSpec(memory_space=pl.ANY)] * len(arrays),
        out_specs=VMEM,
        scratch_shapes=[pltpu.SemaphoreType.DMA((parts * len(arrays),))],
        cost_estimate=pl.CostEstimate(flops=rows * width, bytes_accessed=4 * rows * width, transcendentals=0),
    )(*arrays)


def unpack_body(parts, i_ref, *refs):
    outs, sems = refs[:-1], refs[-1]
    copies = []
    for part in range(parts):
        start = 0
        for ref in outs:
            width = ref.shape[1] // parts
            source, target = i_ref.at[part, :, pl.ds(start, width)], ref.at[:, pl.ds(part * width, width)]
            copies.append(pltpu.make_async_copy(source, target, sems.at[len(copies)]))
            start += width
    run(copies)


def unpack(value, widths):
    parts, rows, _ = value.shape
    return pl.pallas_call(
        functools.partial(unpack_body, parts),
        out_shape=tuple(jax.ShapeDtypeStruct((rows, parts * width), value.dtype) for width in widths),
        in_specs=[VMEM],
        out_specs=(pl.BlockSpec(memory_space=pl.ANY),) * len(widths),
        scratch_shapes=[pltpu.SemaphoreType.DMA((parts * len(widths),))],
        compiler_params=SMALL,
        cost_estimate=pl.CostEstimate(flops=value.size, bytes_accessed=4 * value.size, transcendentals=0),
    )(value)


def add_cut_body(parts, at_ref, base_ref, one_ref, two_ref, three_ref, *o_refs):
    rows = o_refs[0].shape[0]
    for k in range(parts):
        source = pl.ds(pl.multiple_of(lax.rem(at_ref[0] + k, parts) * rows, rows), rows)
        total = base_ref[source, :] + one_ref[source, :].astype(jnp.float32)
        total = total + two_ref[source, :].astype(jnp.float32) + three_ref[source, :].astype(jnp.float32)
        o_refs[k][...] = total.astype(jnp.bfloat16)


def add_cut(at, base, others, parts):
    rows, columns = base.shape[0] // parts, base.shape[1]
    piece = jax.ShapeDtypeStruct((rows, columns), jnp.bfloat16)
    return pl.pallas_call(
        functools.partial(add_cut_body, parts),
        out_shape=(piece,) * parts,
        in_specs=[SMEM] + [VMEM] * 4,
        out_specs=(VMEM,) * parts,
        compiler_params=SMALL,
        cost_estimate=pl.CostEstimate(flops=4 * base.size, bytes_accessed=12 * base.size, transcendentals=0),
        name="add_cut",
    )(at, base, *others)


def join_body(parts, at_ref, *refs):
    a_ref, b_ref = refs[parts:]
    for k in range(parts):
        target = pl.ds(pl.multiple_of(lax.rem(at_ref[0] + (parts - k), parts) * HEAD, HEAD), HEAD)
        a_ref[:, target] = refs[k][:, :HEAD]
        b_ref[:, target] = refs[k][:, HEAD:]


def join(at, pieces):
    parts, rows = len(pieces), pieces[0].shape[0]
    out = jax.ShapeDtypeStruct((rows, parts * HEAD), pieces[0].dtype)
    return pl.pallas_call(
        functools.partial(join_body, parts),
        out_shape=(out, out),
        in_specs=[SMEM] + [VMEM] * parts,
        out_specs=(VMEM, VMEM),
        compiler_params=SMALL,
        cost_estimate=pl.CostEstimate(flops=out.size, bytes_accessed=8 * out.size, transcendentals=0),
        name="join",
    )(at, *pieces)


def prepare(core, own, two, four, six, mate, k_s, v_s, kt_s, vt_s, bias_s, dk_s, dv_s):
    first = 1 - core
    docs = []
    for c in range(CHUNKS):
        if c < SLOTS:
            ref = (own, two, four, six)[c]
            rows, doc = ref[:BLOCK, :], ref[BLOCK:, :]
        else:
            slot = first + (c - SLOTS)
            rows, doc = mate[slot, :BLOCK, :], mate[slot, BLOCK:, :]
        docs.append(doc[0:1, :].astype(jnp.float32))
        key, value = rows[:, :HEAD], rows[:, HEAD:]
        k_s[c] = key
        v_s[c] = value
        kt_s[c] = key.astype(jnp.float32).T.astype(jnp.bfloat16)
        vt_s[c] = value.astype(jnp.float32).T.astype(jnp.bfloat16)
    mine = docs[0]
    by_key = jnp.broadcast_to(mine, (BLOCK, BLOCK)).T
    row = lax.broadcasted_iota(jnp.int32, (BLOCK, BLOCK), 0)
    lane = lax.broadcasted_iota(jnp.int32, (BLOCK, BLOCK), 1)
    before = jnp.sum(jnp.where((by_key == mine) & (row < lane), 1.0, 0.0), axis=0, keepdims=True)
    opening = mine[:, 0:1]
    carried = jnp.zeros((1, 1), jnp.float32)
    for c in range(1, CHUNKS):
        carried = carried + jnp.sum(jnp.where(docs[c] == opening, 1.0, 0.0), axis=1, keepdims=True)
    before = before + jnp.where(mine == opening, carried, 0.0)
    before = jnp.minimum(before, WINDOW - 1.0).astype(jnp.int32)
    for c in range(CHUNKS):
        back = lane - row + OFFSETS[c] * BLOCK
        bias_s[c] = jnp.where((back >= 0) & (back <= before), 0.0, MASKED)
    dk_s[...] = jnp.zeros_like(dk_s)
    dv_s[...] = jnp.zeros_like(dv_s)


def scores(query, s_ref, k_s, bias_s):
    top = None
    for c in range(CHUNKS):
        s = dot(k_s[c], query, NT) * EXP2_SCALE + bias_s[c]
        s_ref[c] = s
        most = jnp.max(s, axis=0, keepdims=True)
        top = most if top is None else jnp.maximum(top, most)
    return top


def weigh(c, s_ref, top, total):
    for r in range(0, BLOCK, PIECE):
        p = jnp.exp2(s_ref[c, r : r + PIECE, :] - top)
        s_ref[c, r : r + PIECE, :] = p
        part = jnp.sum(p, axis=0, keepdims=True)
        total = part if total is None else total + part
    return total


def collect(grad, s_ref, total, y_ref, columns, stat_ref, vt_s, dv_s):
    inverse = 1.0 / total
    out = None
    for c in range(CHUNKS):
        p16 = (s_ref[c] * inverse).astype(jnp.bfloat16)
        term = dot(vt_s[c], p16)
        out = term if out is None else out + term
        dv_s[c] += dot(p16, grad)
    out16 = out.astype(jnp.bfloat16).astype(jnp.float32)
    y_ref[:, columns] = out16.T.astype(jnp.bfloat16)
    delta = jnp.sum(grad.astype(jnp.float32).T * out16, axis=0, keepdims=True)
    stat_ref[0:1, :] = inverse
    stat_ref[1:2, :] = delta


def step(ahead, behind, x_ref, y_ref, k_s, v_s, kt_s, vt_s, bias_s, dk_s, dv_s):
    heads = x_ref.shape[1] // (2 * HEAD)
    first = lambda head: pl.ds(pl.multiple_of(head * HEAD, HEAD), HEAD)
    second = lambda head: pl.ds(pl.multiple_of((heads + head) * HEAD, HEAD), HEAD)
    total = dq = None
    if ahead:
        head, s_ref, stat_ref = ahead
        grad = x_ref[:, second(head)]
        top = scores(x_ref[:, first(head)], s_ref, k_s, bias_s)
    if behind:
        last, p_ref, last_ref = behind
        last_query, last_grad = x_ref[:, first(last)], x_ref[:, second(last)]
        inverse, delta = last_ref[0:1, :], last_ref[1:2, :]
        coming = dot(v_s[0], last_grad, NT)
    for c in range(CHUNKS):
        if behind:
            dp = coming
            if c + 1 < CHUNKS:
                coming = dot(v_s[c + 1], last_grad, NT)
        if ahead:
            total = weigh(c, s_ref, top, total)
        if behind:
            ds = (p_ref[c] * ((dp - delta) * inverse)).astype(jnp.bfloat16)
            term = dot(kt_s[c], ds)
            dq = term if dq is None else dq + term
            dk_s[c] += dot(ds, last_query)
    if behind:
        y_ref[:, second(last)] = (dq * SCALE).T.astype(jnp.bfloat16)
    if ahead:
        collect(grad, s_ref, total, y_ref, first(head), stat_ref, vt_s, dv_s)


def attention_body(core_ref, x_ref, own, two, four, six, mate, y_ref, mine_ref, mate_ref, k_s, v_s, kt_s, vt_s, bias_s, dk_s, dv_s, even_s, odd_s, even_t, odd_t):
    core = core_ref[0]
    heads = x_ref.shape[1] // (2 * HEAD)
    prepare(core, own, two, four, six, mate, k_s, v_s, kt_s, vt_s, bias_s, dk_s, dv_s)
    refs = (x_ref, y_ref, k_s, v_s, kt_s, vt_s, bias_s, dk_s, dv_s)
    step((0, even_s, even_t), None, *refs)

    def pair(i, _):
        head = 2 * i
        step((head + 1, odd_s, odd_t), (head, even_s, even_t), *refs)
        step((head + 2, even_s, even_t), (head + 1, odd_s, odd_t), *refs)
        return 0

    lax.fori_loop(0, heads // 2 - 1, pair, 0)
    step((heads - 1, odd_s, odd_t), (heads - 2, even_s, even_t), *refs)
    step(None, (heads - 1, odd_s, odd_t), *refs)
    for t in range(SLOTS):
        mine_ref[t, :, :HEAD] = dk_s[t] * SCALE
        mine_ref[t, :, HEAD:] = dv_s[t]
    first = 1 - core
    mate_ref[3 - 3 * first] = jnp.zeros((BLOCK, 2 * HEAD), jnp.bfloat16)
    for t in range(SLOTS - 1):
        mate_ref[first + t, :, :HEAD] = (dk_s[SLOTS + t] * SCALE).astype(jnp.bfloat16)
        mate_ref[first + t, :, HEAD:] = dv_s[SLOTS + t].astype(jnp.bfloat16)


def attention(core, x, own, two, four, six, mate):
    heads = x.shape[1] // (2 * HEAD)
    work = heads * CHUNKS * BLOCK * BLOCK
    return pl.pallas_call(
        attention_body,
        out_shape=(
            jax.ShapeDtypeStruct(x.shape, jnp.bfloat16),
            jax.ShapeDtypeStruct((SLOTS, BLOCK, 2 * HEAD), jnp.float32),
            jax.ShapeDtypeStruct((SLOTS, BLOCK, 2 * HEAD), jnp.bfloat16),
        ),
        in_specs=[SMEM] + [VMEM] * 6,
        out_specs=(VMEM,) * 3,
        scratch_shapes=[
            pltpu.VMEM((CHUNKS, BLOCK, HEAD), jnp.bfloat16),
            pltpu.VMEM((CHUNKS, BLOCK, HEAD), jnp.bfloat16),
            pltpu.VMEM((CHUNKS, HEAD, BLOCK), jnp.bfloat16),
            pltpu.VMEM((CHUNKS, HEAD, BLOCK), jnp.bfloat16),
            pltpu.VMEM((CHUNKS, BLOCK, BLOCK), jnp.float32),
            pltpu.VMEM((CHUNKS, BLOCK, HEAD), jnp.float32),
            pltpu.VMEM((CHUNKS, BLOCK, HEAD), jnp.float32),
            pltpu.VMEM((CHUNKS, BLOCK, BLOCK), jnp.float32),
            pltpu.VMEM((CHUNKS, BLOCK, BLOCK), jnp.float32),
            pltpu.VMEM((8, BLOCK), jnp.float32),
            pltpu.VMEM((8, BLOCK), jnp.float32),
        ],
        compiler_params=pltpu.CompilerParams(vmem_limit_bytes=16 * 1024 * 1024),
        cost_estimate=pl.CostEstimate(flops=12 * work * HEAD, bytes_accessed=5 * 1024 * 1024, transcendentals=work),
        name="attention",
    )(core, x, own, two, four, six, mate)


def shift(value, steps):
    count = lax.axis_size("ctx")
    return lax.ppermute(value, "ctx", [(s, s + steps) for s in range(max(0, -steps), min(count, count - steps))])


def swap(value):
    count = lax.axis_size("ctx")
    return lax.ppermute(value, "ctx", [(s, s ^ 1) for s in range(count)])


def over_head(value):
    return lax.all_to_all(value, "head", split_axis=0, concat_axis=0, tiled=True)


def around(value, steps):
    count = lax.axis_size("head")
    return lax.ppermute(value, "head", [(s, (s + steps) % count) for s in range(count)])


def local(queries, key_heads, value_head_array, out_grad, doc_ids):
    parts = lax.axis_size("head")
    core = (lax.axis_index("ctx") % 2).astype(jnp.int32).reshape(1)
    at = lax.axis_index("head").astype(jnp.int32).reshape(1)
    kv = over_head(pack((key_heads, value_head_array), parts)).reshape(BLOCK, -1)
    docs = jnp.pad((doc_ids + 1).astype(jnp.bfloat16)[None, :], ((0, DOC_ROWS - 1), (0, 0)))
    own = jnp.concatenate([kv, docs], axis=0)
    packed = pack((queries, out_grad), parts)
    x = over_head(packed).reshape(BLOCK, -1)
    two, four, six = (shift(own, steps) for steps in (2, 4, 6))
    mate = swap(jnp.stack([own, two, four, six]))
    y, mine, sent = attention(core, x, own, two, four, six, mate)
    sent = swap(sent)
    y = over_head(y.reshape(parts, -1, y.shape[1]))
    sums = mine + sent.astype(jnp.float32)
    rounded = sums.astype(jnp.bfloat16)
    back = [shift(rounded[t], -2 * t) for t in range(1, SLOTS)]
    pieces = add_cut(at, sums[0], back, parts)
    pieces = [pieces[0]] + [around(piece, k) for k, piece in enumerate(pieces) if k]
    attended, query_grad = unpack(y, (y.shape[2] // 2,) * 2)
    key_grad, value_grad = join(at, pieces)
    return attended, query_grad, key_grad, value_grad


def solution(mesh):
    rows = P(("ctx", "head"), None)

    return jax.shard_map(
        local,
        mesh=mesh,
        in_specs=(rows, rows, rows, rows, P("ctx")),
        out_specs=(rows, rows, rows, rows),
        check_vma=False,
    )
```

```python
import functools
import math

import jax
import jax.numpy as jnp
from jax import lax
from jax.experimental import pallas as pl
from jax.experimental.pallas import tpu as pltpu
from jax.sharding import PartitionSpec as P


HEAD = 128
WINDOW = 1536
BLOCK = 256
SLOTS = 4
OFFSETS = (0, 2, 4, 6, 1, 3, 5)
CHUNKS = len(OFFSETS)
DOC_ROWS = 16
PIECE = 64
SCALE = HEAD ** (-0.5)
EXP2_SCALE = SCALE * math.log2(math.e)
MASKED = -1e30
NT = (((1,), (1,)), ((), ()))
VMEM = pl.BlockSpec(memory_space=pltpu.VMEM)
SMEM = pl.BlockSpec(memory_space=pltpu.SMEM)
SMALL = pltpu.CompilerParams(vmem_limit_bytes=8 * 1024 * 1024)


def dot(a, b, dims=(((1,), (0,)), ((), ()))):
    return lax.dot_general(a, b, dims, preferred_element_type=jnp.float32)


def run(copies):
    for copy in copies:
        copy.start()
    for copy in copies:
        copy.wait()


def pack_body(parts, *refs):
    ins, o_ref, sems = refs[:-2], refs[-2], refs[-1]
    copies = []
    for part in range(parts):
        start = 0
        for ref in ins:
            width = ref.shape[1] // parts
            source, target = ref.at[:, pl.ds(part * width, width)], o_ref.at[part, :, pl.ds(start, width)]
            copies.append(pltpu.make_async_copy(source, target, sems.at[len(copies)]))
            start += width
    run(copies)


def pack(arrays, parts):
    rows, width = arrays[0].shape[0], sum(a.shape[1] for a in arrays)
    return pl.pallas_call(
        functools.partial(pack_body, parts),
        out_shape=jax.ShapeDtypeStruct((parts, rows, width // parts), arrays[0].dtype),
        in_specs=[pl.BlockSpec(memory_space=pl.ANY)] * len(arrays),
        out_specs=VMEM,
        scratch_shapes=[pltpu.SemaphoreType.DMA((parts * len(arrays),))],
        cost_estimate=pl.CostEstimate(flops=rows * width, bytes_accessed=4 * rows * width, transcendentals=0),
    )(*arrays)


def unpack_body(parts, i_ref, *refs):
    outs, sems = refs[:-1], refs[-1]
    copies = []
    for part in range(parts):
        start = 0
        for ref in outs:
            width = ref.shape[1] // parts
            source, target = i_ref.at[part, :, pl.ds(start, width)], ref.at[:, pl.ds(part * width, width)]
            copies.append(pltpu.make_async_copy(source, target, sems.at[len(copies)]))
            start += width
    run(copies)


def unpack(value, widths):
    parts, rows, _ = value.shape
    return pl.pallas_call(
        functools.partial(unpack_body, parts),
        out_shape=tuple(jax.ShapeDtypeStruct((rows, parts * width), value.dtype) for width in widths),
        in_specs=[VMEM],
        out_specs=(pl.BlockSpec(memory_space=pl.ANY),) * len(widths),
        scratch_shapes=[pltpu.SemaphoreType.DMA((parts * len(widths),))],
        compiler_params=SMALL,
        cost_estimate=pl.CostEstimate(flops=value.size, bytes_accessed=4 * value.size, transcendentals=0),
    )(value)


def add_cut_body(parts, at_ref, base_ref, one_ref, two_ref, three_ref, *o_refs):
    rows = o_refs[0].shape[0]
    for k in range(parts):
        source = pl.ds(pl.multiple_of(lax.rem(at_ref[0] + k, parts) * rows, rows), rows)
        total = base_ref[source, :] + one_ref[source, :].astype(jnp.float32)
        total = total + two_ref[source, :].astype(jnp.float32) + three_ref[source, :].astype(jnp.float32)
        o_refs[k][...] = total.astype(jnp.bfloat16)


def add_cut(at, base, others, parts):
    rows, columns = base.shape[0] // parts, base.shape[1]
    piece = jax.ShapeDtypeStruct((rows, columns), jnp.bfloat16)
    return pl.pallas_call(
        functools.partial(add_cut_body, parts),
        out_shape=(piece,) * parts,
        in_specs=[SMEM] + [VMEM] * 4,
        out_specs=(VMEM,) * parts,
        compiler_params=SMALL,
        cost_estimate=pl.CostEstimate(flops=4 * base.size, bytes_accessed=12 * base.size, transcendentals=0),
        name="add_cut",
    )(at, base, *others)


def join_body(parts, at_ref, *refs):
    a_ref, b_ref = refs[parts:]
    for k in range(parts):
        target = pl.ds(pl.multiple_of(lax.rem(at_ref[0] + (parts - k), parts) * HEAD, HEAD), HEAD)
        a_ref[:, target] = refs[k][:, :HEAD]
        b_ref[:, target] = refs[k][:, HEAD:]


def join(at, pieces):
    parts, rows = len(pieces), pieces[0].shape[0]
    out = jax.ShapeDtypeStruct((rows, parts * HEAD), pieces[0].dtype)
    return pl.pallas_call(
        functools.partial(join_body, parts),
        out_shape=(out, out),
        in_specs=[SMEM] + [VMEM] * parts,
        out_specs=(VMEM, VMEM),
        compiler_params=SMALL,
        cost_estimate=pl.CostEstimate(flops=out.size, bytes_accessed=8 * out.size, transcendentals=0),
        name="join",
    )(at, *pieces)


def prepare(core, own, two, four, six, mate, k_s, v_s, kt_s, vt_s, bias_s, dk_s, dv_s):
    first = 1 - core
    docs = []
    for c in range(CHUNKS):
        if c < SLOTS:
            ref = (own, two, four, six)[c]
            rows, doc = ref[:BLOCK, :], ref[BLOCK:, :]
        else:
            slot = first + (c - SLOTS)
            rows, doc = mate[slot, :BLOCK, :], mate[slot, BLOCK:, :]
        docs.append(doc[0:1, :].astype(jnp.float32))
        key, value = rows[:, :HEAD], rows[:, HEAD:]
        k_s[c] = key
        v_s[c] = value
        kt_s[c] = key.astype(jnp.float32).T.astype(jnp.bfloat16)
        vt_s[c] = value.astype(jnp.float32).T.astype(jnp.bfloat16)
    mine = docs[0]
    by_key = jnp.broadcast_to(mine, (BLOCK, BLOCK)).T
    row = lax.broadcasted_iota(jnp.int32, (BLOCK, BLOCK), 0)
    lane = lax.broadcasted_iota(jnp.int32, (BLOCK, BLOCK), 1)
    before = jnp.sum(jnp.where((by_key == mine) & (row < lane), 1.0, 0.0), axis=0, keepdims=True)
    opening = mine[:, 0:1]
    carried = jnp.zeros((1, 1), jnp.float32)
    for c in range(1, CHUNKS):
        carried = carried + jnp.sum(jnp.where(docs[c] == opening, 1.0, 0.0), axis=1, keepdims=True)
    before = before + jnp.where(mine == opening, carried, 0.0)
    before = jnp.minimum(before, WINDOW - 1.0).astype(jnp.int32)
    for c in range(CHUNKS):
        back = lane - row + OFFSETS[c] * BLOCK
        bias_s[c] = jnp.where((back >= 0) & (back <= before), 0.0, MASKED)
    dk_s[...] = jnp.zeros_like(dk_s)
    dv_s[...] = jnp.zeros_like(dv_s)


def scores(query, s_ref, k_s, bias_s):
    top = None
    for c in range(CHUNKS):
        s = dot(k_s[c], query, NT) * EXP2_SCALE + bias_s[c]
        s_ref[c] = s
        most = jnp.max(s, axis=0, keepdims=True)
        top = most if top is None else jnp.maximum(top, most)
    return top


def weigh(c, s_ref, top, total):
    whole = []
    for r in range(0, BLOCK, PIECE):
        p = jnp.exp2(s_ref[c, r : r + PIECE, :] - top)
        s_ref[c, r : r + PIECE, :] = p
        part = jnp.sum(p, axis=0, keepdims=True)
        total = part if total is None else total + part
        whole.append(p.astype(jnp.bfloat16))
    return total, jnp.concatenate(whole, axis=0)


def step(ahead, behind, x_ref, y_ref, k_s, v_s, kt_s, vt_s, bias_s, dk_s, dv_s):
    heads = x_ref.shape[1] // (2 * HEAD)
    first = lambda head: pl.ds(pl.multiple_of(head * HEAD, HEAD), HEAD)
    second = lambda head: pl.ds(pl.multiple_of((heads + head) * HEAD, HEAD), HEAD)
    total = out = dq = None
    if ahead:
        head, s_ref, g_ref, sum_ref = ahead
        top = scores(x_ref[:, first(head)], s_ref, k_s, bias_s)
    if behind:
        last, p_ref, last_ref, delta_ref = behind
        query, grad = x_ref[:, first(last)], last_ref[...]
        delta = delta_ref[0:1, :]
        coming = dot(v_s[0], grad, NT)
    for c in range(CHUNKS):
        if behind:
            dp = coming
            if c + 1 < CHUNKS:
                coming = dot(v_s[c + 1], grad, NT)
        if ahead:
            total, p16 = weigh(c, s_ref, top, total)
            term = dot(vt_s[c], p16)
            out = term if out is None else out + term
        if behind:
            p = p_ref[c]
            ds = (p * (dp - delta)).astype(jnp.bfloat16)
            term = dot(kt_s[c], ds)
            dq = term if dq is None else dq + term
            dk_s[c] += dot(ds, query)
            dv_s[c] += dot(p.astype(jnp.bfloat16), grad)
    if behind:
        y_ref[:, second(last)] = (dq * SCALE).T.astype(jnp.bfloat16)
    if ahead:
        inverse = 1.0 / total
        out16 = (out * inverse).astype(jnp.bfloat16).astype(jnp.float32)
        y_ref[:, first(head)] = out16.T.astype(jnp.bfloat16)
        full = x_ref[:, second(head)].astype(jnp.float32)
        sum_ref[0:1, :] = jnp.sum(full.T * out16, axis=0, keepdims=True) * inverse
        g_ref[...] = (full * jnp.broadcast_to(inverse, (HEAD, BLOCK)).T).astype(jnp.bfloat16)


def attention_body(core_ref, x_ref, own, two, four, six, mate, y_ref, mine_ref, mate_ref, k_s, v_s, kt_s, vt_s, bias_s, dk_s, dv_s, even_s, odd_s, even_g, odd_g, even_t, odd_t):
    core = core_ref[0]
    heads = x_ref.shape[1] // (2 * HEAD)
    prepare(core, own, two, four, six, mate, k_s, v_s, kt_s, vt_s, bias_s, dk_s, dv_s)
    refs = (x_ref, y_ref, k_s, v_s, kt_s, vt_s, bias_s, dk_s, dv_s)
    step((0, even_s, even_g, even_t), None, *refs)

    def pair(i, _):
        head = 2 * i
        step((head + 1, odd_s, odd_g, odd_t), (head, even_s, even_g, even_t), *refs)
        step((head + 2, even_s, even_g, even_t), (head + 1, odd_s, odd_g, odd_t), *refs)
        return 0

    lax.fori_loop(0, heads // 2 - 1, pair, 0)
    step((heads - 1, odd_s, odd_g, odd_t), (heads - 2, even_s, even_g, even_t), *refs)
    step(None, (heads - 1, odd_s, odd_g, odd_t), *refs)
    for t in range(SLOTS):
        mine_ref[t, :, :HEAD] = dk_s[t] * SCALE
        mine_ref[t, :, HEAD:] = dv_s[t]
    first = 1 - core
    mate_ref[3 - 3 * first] = jnp.zeros((BLOCK, 2 * HEAD), jnp.bfloat16)
    for t in range(SLOTS - 1):
        mate_ref[first + t, :, :HEAD] = (dk_s[SLOTS + t] * SCALE).astype(jnp.bfloat16)
        mate_ref[first + t, :, HEAD:] = dv_s[SLOTS + t].astype(jnp.bfloat16)


def attention(core, x, own, two, four, six, mate):
    heads = x.shape[1] // (2 * HEAD)
    work = heads * CHUNKS * BLOCK * BLOCK
    return pl.pallas_call(
        attention_body,
        out_shape=(
            jax.ShapeDtypeStruct(x.shape, jnp.bfloat16),
            jax.ShapeDtypeStruct((SLOTS, BLOCK, 2 * HEAD), jnp.float32),
            jax.ShapeDtypeStruct((SLOTS, BLOCK, 2 * HEAD), jnp.bfloat16),
        ),
        in_specs=[SMEM] + [VMEM] * 6,
        out_specs=(VMEM,) * 3,
        scratch_shapes=[
            pltpu.VMEM((CHUNKS, BLOCK, HEAD), jnp.bfloat16),
            pltpu.VMEM((CHUNKS, BLOCK, HEAD), jnp.bfloat16),
            pltpu.VMEM((CHUNKS, HEAD, BLOCK), jnp.bfloat16),
            pltpu.VMEM((CHUNKS, HEAD, BLOCK), jnp.bfloat16),
            pltpu.VMEM((CHUNKS, BLOCK, BLOCK), jnp.float32),
            pltpu.VMEM((CHUNKS, BLOCK, HEAD), jnp.float32),
            pltpu.VMEM((CHUNKS, BLOCK, HEAD), jnp.float32),
            pltpu.VMEM((CHUNKS, BLOCK, BLOCK), jnp.float32),
            pltpu.VMEM((CHUNKS, BLOCK, BLOCK), jnp.float32),
            pltpu.VMEM((BLOCK, HEAD), jnp.bfloat16),
            pltpu.VMEM((BLOCK, HEAD), jnp.bfloat16),
            pltpu.VMEM((8, BLOCK), jnp.float32),
            pltpu.VMEM((8, BLOCK), jnp.float32),
        ],
        compiler_params=pltpu.CompilerParams(vmem_limit_bytes=16 * 1024 * 1024),
        cost_estimate=pl.CostEstimate(flops=12 * work * HEAD, bytes_accessed=5 * 1024 * 1024, transcendentals=work),
        name="attention",
    )(core, x, own, two, four, six, mate)


def shift(value, steps):
    count = lax.axis_size("ctx")
    return lax.ppermute(value, "ctx", [(s, s + steps) for s in range(max(0, -steps), min(count, count - steps))])


def swap(value):
    count = lax.axis_size("ctx")
    return lax.ppermute(value, "ctx", [(s, s ^ 1) for s in range(count)])


def over_head(value):
    return lax.all_to_all(value, "head", split_axis=0, concat_axis=0, tiled=True)


def around(value, steps):
    count = lax.axis_size("head")
    return lax.ppermute(value, "head", [(s, (s + steps) % count) for s in range(count)])


def local(queries, key_heads, value_head_array, out_grad, doc_ids):
    parts = lax.axis_size("head")
    core = (lax.axis_index("ctx") % 2).astype(jnp.int32).reshape(1)
    at = lax.axis_index("head").astype(jnp.int32).reshape(1)
    kv = over_head(pack((key_heads, value_head_array), parts)).reshape(BLOCK, -1)
    docs = jnp.pad((doc_ids + 1).astype(jnp.bfloat16)[None, :], ((0, DOC_ROWS - 1), (0, 0)))
    own = jnp.concatenate([kv, docs], axis=0)
    packed = pack((queries, out_grad), parts)
    x = over_head(packed).reshape(BLOCK, -1)
    two, four, six = (shift(own, steps) for steps in (2, 4, 6))
    mate = swap(jnp.stack([own, two, four, six]))
    y, mine, sent = attention(core, x, own, two, four, six, mate)
    sent = swap(sent)
    y = over_head(y.reshape(parts, -1, y.shape[1]))
    sums = mine + sent.astype(jnp.float32)
    rounded = sums.astype(jnp.bfloat16)
    back = []
    for t in range(1, SLOTS):
        back.append(shift(rounded[t], -2 * t))
    pieces = add_cut(at, sums[0], back, parts)
    pieces = [pieces[0]] + [around(piece, k) for k, piece in enumerate(pieces) if k]
    attended, query_grad = unpack(y, (y.shape[2] // 2,) * 2)
    key_grad, value_grad = join(at, pieces)
    return attended, query_grad, key_grad, value_grad


def solution(mesh):
    rows = P(("ctx", "head"), None)

    return jax.shard_map(
        local,
        mesh=mesh,
        in_specs=(rows, rows, rows, rows, P("ctx")),
        out_specs=(rows, rows, rows, rows),
        check_vma=False,
    )
```

```python
import functools
import math

import jax
import jax.numpy as jnp
from jax import lax
from jax.experimental import pallas as pl
from jax.experimental.pallas import tpu as pltpu
from jax.sharding import PartitionSpec as P


HEAD = 128
WINDOW = 1536
BLOCK = 256
SLOTS = 4
OFFSETS = (0, 2, 4, 6, 1, 3, 5)
CHUNKS = len(OFFSETS)
DOC_ROWS = 16
PIECE = 256
SCALE = HEAD ** (-0.5)
EXP2_SCALE = SCALE * math.log2(math.e)
MASKED = -1e30
NT = (((1,), (1,)), ((), ()))
VMEM = pl.BlockSpec(memory_space=pltpu.VMEM)
SMEM = pl.BlockSpec(memory_space=pltpu.SMEM)
SMALL = pltpu.CompilerParams(vmem_limit_bytes=8 * 1024 * 1024)


def dot(a, b, dims=(((1,), (0,)), ((), ()))):
    return lax.dot_general(a, b, dims, preferred_element_type=jnp.float32)


def run(copies):
    for copy in copies:
        copy.start()
    for copy in copies:
        copy.wait()


def pack_body(parts, *refs):
    ins, o_ref, sems = refs[:-2], refs[-2], refs[-1]
    copies = []
    for part in range(parts):
        start = 0
        for ref in ins:
            width = ref.shape[1] // parts
            source, target = ref.at[:, pl.ds(part * width, width)], o_ref.at[part, :, pl.ds(start, width)]
            copies.append(pltpu.make_async_copy(source, target, sems.at[len(copies)]))
            start += width
    run(copies)


def pack(arrays, parts):
    rows, width = arrays[0].shape[0], sum(a.shape[1] for a in arrays)
    return pl.pallas_call(
        functools.partial(pack_body, parts),
        out_shape=jax.ShapeDtypeStruct((parts, rows, width // parts), arrays[0].dtype),
        in_specs=[pl.BlockSpec(memory_space=pl.ANY)] * len(arrays),
        out_specs=VMEM,
        scratch_shapes=[pltpu.SemaphoreType.DMA((parts * len(arrays),))],
        cost_estimate=pl.CostEstimate(flops=rows * width, bytes_accessed=4 * rows * width, transcendentals=0),
    )(*arrays)


def unpack_body(parts, i_ref, *refs):
    outs, sems = refs[:-1], refs[-1]
    copies = []
    for part in range(parts):
        start = 0
        for ref in outs:
            width = ref.shape[1] // parts
            source, target = i_ref.at[part, :, pl.ds(start, width)], ref.at[:, pl.ds(part * width, width)]
            copies.append(pltpu.make_async_copy(source, target, sems.at[len(copies)]))
            start += width
    run(copies)


def unpack(value, widths):
    parts, rows, _ = value.shape
    return pl.pallas_call(
        functools.partial(unpack_body, parts),
        out_shape=tuple(jax.ShapeDtypeStruct((rows, parts * width), value.dtype) for width in widths),
        in_specs=[VMEM],
        out_specs=(pl.BlockSpec(memory_space=pl.ANY),) * len(widths),
        scratch_shapes=[pltpu.SemaphoreType.DMA((parts * len(widths),))],
        compiler_params=SMALL,
        cost_estimate=pl.CostEstimate(flops=value.size, bytes_accessed=4 * value.size, transcendentals=0),
    )(value)


def pair_body(mine_ref, sent_ref, base_ref, *o_refs):
    base_ref[...] = mine_ref[0] + sent_ref[0].astype(jnp.float32)
    for t, o_ref in enumerate(o_refs):
        o_ref[...] = (mine_ref[t + 1] + sent_ref[t + 1].astype(jnp.float32)).astype(jnp.bfloat16)


def pair(mine, sent):
    slots, rows, columns = mine.shape
    block = lambda kind: jax.ShapeDtypeStruct((rows, columns), kind)
    return pl.pallas_call(
        pair_body,
        out_shape=(block(jnp.float32),) + (block(jnp.bfloat16),) * (slots - 1),
        in_specs=[VMEM] * 2,
        out_specs=(VMEM,) * slots,
        compiler_params=SMALL,
        cost_estimate=pl.CostEstimate(flops=mine.size, bytes_accessed=8 * mine.size, transcendentals=0),
        name="pair",
    )(mine, sent)


def add_cut_body(parts, at_ref, base_ref, one_ref, two_ref, three_ref, *o_refs):
    rows = o_refs[0].shape[0]
    for k in range(parts):
        source = pl.ds(pl.multiple_of(lax.rem(at_ref[0] + k, parts) * rows, rows), rows)
        total = base_ref[source, :] + one_ref[source, :].astype(jnp.float32)
        total = total + two_ref[source, :].astype(jnp.float32) + three_ref[source, :].astype(jnp.float32)
        o_refs[k][...] = total.astype(jnp.bfloat16)


def add_cut(at, base, others, parts):
    rows, columns = base.shape[0] // parts, base.shape[1]
    piece = jax.ShapeDtypeStruct((rows, columns), jnp.bfloat16)
    return pl.pallas_call(
        functools.partial(add_cut_body, parts),
        out_shape=(piece,) * parts,
        in_specs=[SMEM] + [VMEM] * 4,
        out_specs=(VMEM,) * parts,
        compiler_params=SMALL,
        cost_estimate=pl.CostEstimate(flops=4 * base.size, bytes_accessed=12 * base.size, transcendentals=0),
        name="add_cut",
    )(at, base, *others)


def join_body(parts, at_ref, *refs):
    a_ref, b_ref = refs[parts:]
    for k in range(parts):
        target = pl.ds(pl.multiple_of(lax.rem(at_ref[0] + (parts - k), parts) * HEAD, HEAD), HEAD)
        a_ref[:, target] = refs[k][:, :HEAD]
        b_ref[:, target] = refs[k][:, HEAD:]


def join(at, pieces):
    parts, rows = len(pieces), pieces[0].shape[0]
    out = jax.ShapeDtypeStruct((rows, parts * HEAD), pieces[0].dtype)
    return pl.pallas_call(
        functools.partial(join_body, parts),
        out_shape=(out, out),
        in_specs=[SMEM] + [VMEM] * parts,
        out_specs=(VMEM, VMEM),
        compiler_params=SMALL,
        cost_estimate=pl.CostEstimate(flops=out.size, bytes_accessed=8 * out.size, transcendentals=0),
        name="join",
    )(at, *pieces)


def prepare(core, own, two, four, six, mate, k_s, v_s, kt_s, vt_s, bias_s, dk_s, dv_s):
    first = 1 - core
    docs = []
    for c in range(CHUNKS):
        if c < SLOTS:
            ref = (own, two, four, six)[c]
            rows, doc = ref[:BLOCK, :], ref[BLOCK:, :]
        else:
            slot = first + (c - SLOTS)
            rows, doc = mate[slot, :BLOCK, :], mate[slot, BLOCK:, :]
        docs.append(doc[0:1, :].astype(jnp.float32))
        key, value = rows[:, :HEAD], rows[:, HEAD:]
        k_s[c] = key
        v_s[c] = value
        kt_s[c] = key.T
        vt_s[c] = value.T
    mine = docs[0]
    by_key = jnp.broadcast_to(mine, (BLOCK, BLOCK)).T
    row = lax.broadcasted_iota(jnp.int32, (BLOCK, BLOCK), 0)
    lane = lax.broadcasted_iota(jnp.int32, (BLOCK, BLOCK), 1)
    before = jnp.sum(jnp.where((by_key == mine) & (row < lane), 1.0, 0.0), axis=0, keepdims=True)
    opening = mine[:, 0:1]
    carried = jnp.zeros((1, 1), jnp.float32)
    for c in range(1, CHUNKS):
        carried = carried + jnp.sum(jnp.where(docs[c] == opening, 1.0, 0.0), axis=1, keepdims=True)
    before = before + jnp.where(mine == opening, carried, 0.0)
    before = jnp.minimum(before, WINDOW - 1.0).astype(jnp.int32)
    for c in range(CHUNKS):
        back = lane - row + OFFSETS[c] * BLOCK
        bias_s[c] = jnp.where((back >= 0) & (back <= before), 0.0, MASKED)
    dk_s[...] = jnp.zeros_like(dk_s)
    dv_s[...] = jnp.zeros_like(dv_s)


def scores(query, s_ref, k_s, bias_s):
    top = None
    for c in range(CHUNKS):
        s = dot(k_s[c], query, NT) * EXP2_SCALE + bias_s[c]
        s_ref[c] = s
        most = jnp.max(s, axis=0, keepdims=True)
        top = most if top is None else jnp.maximum(top, most)
    return top


def weigh(c, s_ref, top, total):
    whole = []
    for r in range(0, BLOCK, PIECE):
        p = jnp.exp2(s_ref[c, r : r + PIECE, :] - top)
        s_ref[c, r : r + PIECE, :] = p
        part = jnp.sum(p, axis=0, keepdims=True)
        total = part if total is None else total + part
        whole.append(p.astype(jnp.bfloat16))
    return total, jnp.concatenate(whole, axis=0)


def step(ahead, behind, x_ref, y_ref, k_s, v_s, kt_s, vt_s, bias_s, dk_s, dv_s):
    heads = x_ref.shape[1] // (2 * HEAD)
    first = lambda head: pl.ds(pl.multiple_of(head * HEAD, HEAD), HEAD)
    second = lambda head: pl.ds(pl.multiple_of((heads + head) * HEAD, HEAD), HEAD)
    total = out = dq = None
    if ahead:
        head, s_ref, g_ref, sum_ref = ahead
        top = scores(x_ref[:, first(head)], s_ref, k_s, bias_s)
    if behind:
        last, p_ref, last_ref, delta_ref = behind
        query, grad = x_ref[:, first(last)], last_ref[...]
        delta = delta_ref[0:1, :]
        coming = dot(v_s[0], grad, NT)
    for c in range(CHUNKS):
        if behind:
            dp = coming
            if c + 1 < CHUNKS:
                coming = dot(v_s[c + 1], grad, NT)
        if ahead:
            total, p16 = weigh(c, s_ref, top, total)
            term = dot(vt_s[c], p16)
            out = term if out is None else out + term
        if behind:
            p = p_ref[c]
            ds = (p * (dp - delta)).astype(jnp.bfloat16)
            term = dot(kt_s[c], ds)
            dq = term if dq is None else dq + term
            dk_s[c] += dot(ds, query)
            dv_s[c] += dot(p.astype(jnp.bfloat16), grad)
    if behind:
        y_ref[:, second(last)] = (dq * SCALE).T.astype(jnp.bfloat16)
    if ahead:
        inverse = 1.0 / total
        out16 = (out * inverse).astype(jnp.bfloat16).astype(jnp.float32)
        y_ref[:, first(head)] = out16.T.astype(jnp.bfloat16)
        full = x_ref[:, second(head)].astype(jnp.float32)
        sum_ref[0:1, :] = jnp.sum(full.T * out16, axis=0, keepdims=True) * inverse
        g_ref[...] = (full * jnp.broadcast_to(inverse, (HEAD, BLOCK)).T).astype(jnp.bfloat16)


def attention_body(core_ref, x_ref, own, two, four, six, mate, y_ref, mine_ref, mate_ref, k_s, v_s, kt_s, vt_s, bias_s, dk_s, dv_s, even_s, odd_s, even_g, odd_g, even_t, odd_t):
    core = core_ref[0]
    heads = x_ref.shape[1] // (2 * HEAD)
    prepare(core, own, two, four, six, mate, k_s, v_s, kt_s, vt_s, bias_s, dk_s, dv_s)
    refs = (x_ref, y_ref, k_s, v_s, kt_s, vt_s, bias_s, dk_s, dv_s)
    step((0, even_s, even_g, even_t), None, *refs)

    def pair(i, _):
        head = 2 * i
        step((head + 1, odd_s, odd_g, odd_t), (head, even_s, even_g, even_t), *refs)
        step((head + 2, even_s, even_g, even_t), (head + 1, odd_s, odd_g, odd_t), *refs)
        return 0

    lax.fori_loop(0, heads // 2 - 1, pair, 0)
    step((heads - 1, odd_s, odd_g, odd_t), (heads - 2, even_s, even_g, even_t), *refs)
    step(None, (heads - 1, odd_s, odd_g, odd_t), *refs)
    for t in range(SLOTS):
        mine_ref[t, :, :HEAD] = dk_s[t] * SCALE
        mine_ref[t, :, HEAD:] = dv_s[t]
    first = 1 - core
    mate_ref[3 - 3 * first] = jnp.zeros((BLOCK, 2 * HEAD), jnp.bfloat16)
    for t in range(SLOTS - 1):
        mate_ref[first + t, :, :HEAD] = (dk_s[SLOTS + t] * SCALE).astype(jnp.bfloat16)
        mate_ref[first + t, :, HEAD:] = dv_s[SLOTS + t].astype(jnp.bfloat16)


def attention(core, x, own, two, four, six, mate):
    heads = x.shape[1] // (2 * HEAD)
    work = heads * CHUNKS * BLOCK * BLOCK
    return pl.pallas_call(
        attention_body,
        out_shape=(
            jax.ShapeDtypeStruct(x.shape, jnp.bfloat16),
            jax.ShapeDtypeStruct((SLOTS, BLOCK, 2 * HEAD), jnp.float32),
            jax.ShapeDtypeStruct((SLOTS, BLOCK, 2 * HEAD), jnp.bfloat16),
        ),
        in_specs=[SMEM] + [VMEM] * 6,
        out_specs=(VMEM,) * 3,
        scratch_shapes=[
            pltpu.VMEM((CHUNKS, BLOCK, HEAD), jnp.bfloat16),
            pltpu.VMEM((CHUNKS, BLOCK, HEAD), jnp.bfloat16),
            pltpu.VMEM((CHUNKS, HEAD, BLOCK), jnp.bfloat16),
            pltpu.VMEM((CHUNKS, HEAD, BLOCK), jnp.bfloat16),
            pltpu.VMEM((CHUNKS, BLOCK, BLOCK), jnp.float32),
            pltpu.VMEM((CHUNKS, BLOCK, HEAD), jnp.float32),
            pltpu.VMEM((CHUNKS, BLOCK, HEAD), jnp.float32),
            pltpu.VMEM((CHUNKS, BLOCK, BLOCK), jnp.float32),
            pltpu.VMEM((CHUNKS, BLOCK, BLOCK), jnp.float32),
            pltpu.VMEM((BLOCK, HEAD), jnp.bfloat16),
            pltpu.VMEM((BLOCK, HEAD), jnp.bfloat16),
            pltpu.VMEM((8, BLOCK), jnp.float32),
            pltpu.VMEM((8, BLOCK), jnp.float32),
        ],
        compiler_params=pltpu.CompilerParams(vmem_limit_bytes=16 * 1024 * 1024),
        cost_estimate=pl.CostEstimate(flops=12 * work * HEAD, bytes_accessed=5 * 1024 * 1024, transcendentals=work),
        name="attention",
    )(core, x, own, two, four, six, mate)


def shift(value, steps):
    count = lax.axis_size("ctx")
    return lax.ppermute(value, "ctx", [(s, s + steps) for s in range(max(0, -steps), min(count, count - steps))])


def swap(value):
    count = lax.axis_size("ctx")
    return lax.ppermute(value, "ctx", [(s, s ^ 1) for s in range(count)])


def over_head(value):
    return lax.all_to_all(value, "head", split_axis=0, concat_axis=0, tiled=True)


def around(value, steps):
    count = lax.axis_size("head")
    return lax.ppermute(value, "head", [(s, (s + steps) % count) for s in range(count)])


def local(queries, key_heads, value_head_array, out_grad, doc_ids):
    parts = lax.axis_size("head")
    core = (lax.axis_index("ctx") % 2).astype(jnp.int32).reshape(1)
    at = lax.axis_index("head").astype(jnp.int32).reshape(1)
    kv = over_head(pack((key_heads, value_head_array), parts)).reshape(BLOCK, -1)
    docs = jnp.pad((doc_ids + 1).astype(jnp.bfloat16)[None, :], ((0, DOC_ROWS - 1), (0, 0)))
    own = jnp.concatenate([kv, docs], axis=0)
    packed = pack((queries, out_grad), parts)
    x = over_head(packed).reshape(BLOCK, -1)
    two, four, six = (shift(own, steps) for steps in (2, 4, 6))
    mate = swap(jnp.stack([own, two, four, six]))
    y, mine, sent = attention(core, x, own, two, four, six, mate)
    sent = swap(sent)
    y = over_head(y.reshape(parts, -1, y.shape[1]))
    base, *rounded = pair(mine, sent)
    back = []
    for t in range(1, SLOTS):
        back.append(shift(rounded[t - 1], -2 * t))
    pieces = add_cut(at, base, back, parts)
    far_first = sorted(range(1, parts), key=lambda k: abs(2 * k - parts))
    moved = {k: around(pieces[k], k) for k in far_first}
    pieces = [pieces[0]] + [moved[k] for k in range(1, parts)]
    attended, query_grad = unpack(y, (y.shape[2] // 2,) * 2)
    key_grad, value_grad = join(at, pieces)
    return attended, query_grad, key_grad, value_grad


def solution(mesh):
    rows = P(("ctx", "head"), None)

    return jax.shard_map(
        local,
        mesh=mesh,
        in_specs=(rows, rows, rows, rows, P("ctx")),
        out_specs=(rows, rows, rows, rows),
        check_vma=False,
    )
```
